32 devices in a mesh: ep: 8 (over z, x), dp: 4 (over y, core).
Axes of the slice: x: 2, y: 2, z: 4, core: 2. Of those that a mesh axis runs over, the one named last changes fastest.
Arguments:
- grad_out: float32 [4096, 1536], P(('ep', 'dp')), may hold values from -6 to 6
- tokens: bfloat16 [4096, 1536], P(('ep', 'dp')), may hold values from -6 to 6
- probs: float32 [4096, 4], P(('ep', 'dp')), may hold values from 0.1 to 0.5
- expert_ids: int32 [4096, 4], P(('ep', 'dp')), may hold values from 0 to 7, all different within a row; in each aligned block of 128 rows (0 to 127, 128 to 255, ...) at most 80 rows name the same one
- priority: int32 [32, 128], P(('ep', 'dp')), may hold values from 0 to 127, each once within a row
- cap_counts: int32 [8], replicated, may hold values from 40 to 80, as said below
- gate_weight: bfloat16 [8, 1536, 1536], P('ep'), may hold values from -0.15625 to 0.15625
- up_weight: bfloat16 [8, 1536, 1536], P('ep'), may hold values from -0.15625 to 0.15625
- down_weight: bfloat16 [8, 1536, 1536], P('ep'), may hold values from -0.15625 to 0.15625
Outputs:
- input_grad: bfloat16 [4096, 1536], P(('ep', 'dp'))
- prob_grad: float32 [4096, 4], P(('ep', 'dp'))
- gate_grad: bfloat16 [8, 1536, 1536], P('ep', 'dp')
- up_grad: bfloat16 [8, 1536, 1536], P('ep', 'dp')
- down_grad: bfloat16 [8, 1536, 1536], P('ep', 'dp')
The draws below stay inside these ranges and needn't reach their ends.
Inputs may be any that keep to these rules, and one draw needn't show every extreme that they name: `expert_ids`: each row names 4 different experts; among the rows of one device no expert is named by more than 80 rows, and in some device some expert is named by exactly 80 rows. `priority`: each row orders the 128 tokens of one device, each number once. `cap_counts`: some expert has exactly 80.
All inputs are finite; a program needn't handle non-finite values. Where the reference program divides by a largest or mean magnitude, that divisor is 1e-20 or more.
Results may differ from the reference program's by a relative error of at most 0.017.
Values may be sent and summed in bfloat16 or wider, within the bound.
No kernel may reach another device: no remote copies, remote signals or barrier semaphores. Data moves between devices by JAX's collectives and lax.ppermute only.
A program may use at most 128 MiB of HBM per device.

```python
import math
import jax
import jax.numpy as jnp
import numpy as np
from jax import lax

D = 1536
FH = 1536
TOP = 4
TOK_DEV = 128
EXPERTS = 8
TOKENS = 4096
CAP = 80
N_EP = 8
N_DP = 4


def draw_cap_counts(key, part):
    first_key, second_key = jax.random.split(jax.random.fold_in(key, 17))
    counts = jax.random.randint(first_key, (EXPERTS,), CAP // 2, CAP + 1)
    chosen = jax.random.randint(second_key, (), 0, EXPERTS)
    return jnp.where(jnp.arange(EXPERTS) == chosen, CAP, counts).astype(jnp.int32)


def level_of(own_key, dims, shards, smallest, largest):
    level, own = 1.0, jax.random.fold_in(own_key, 6)
    for dim, shards_of in shards:
        draws = jnp.exp(jax.random.uniform(jax.random.fold_in(own, dim), (shards_of,), jnp.float32, smallest / len(shards), largest / len(shards)))
        level = level * jnp.repeat(draws, dims[dim] // shards_of).reshape([-1 if axis == dim else 1 for axis in range(len(dims))])
    return level


def deal_out(rng, own, number, rows, amount, top, bound, slope):
    order = jax.random.permutation(rng, amount)
    crowded, common = load_shares(amount, rows * top, bound, slope, True), load_shares(amount, rows * top, bound, slope, False)
    places = jnp.arange(amount)

    def named(tallies, rotation):
        used = int((tallies > 0).sum())
        fixed = max(1, used // 4)
        passed = fixed + (places - fixed + rotation * (used - fixed)) % max(1, amount - fixed)
        return jnp.zeros((amount,), jnp.int32).at[order[jnp.where(places < fixed, places, passed)]].set(jnp.asarray(tallies, jnp.int32))

    tallies = jnp.where(number % 4 == 0, named(crowded, number // 4), named(common, number - number // 4 - 1))
    mixed = jax.random.permutation(jax.random.fold_in(own, 3), amount)
    source_of, sink = mixed[0:amount // 2 * 2:2], mixed[1:amount // 2 * 2:2]
    room = jnp.minimum(tallies[source_of] - 1, bound - tallies[sink]) // 2
    room = jnp.where((source_of == order[0]) | (sink == order[0]) | (tallies[sink] == 0), 0, jnp.maximum(room, 0))
    passed = jax.random.randint(jax.random.fold_in(own, 4), (amount // 2,), 0, 1 << 20) % (room + 1)
    tallies = tallies.at[source_of].add(-passed).at[sink].add(passed)
    members = jnp.searchsorted(jnp.cumsum(tallies), jnp.arange(rows * top), side="right").astype(jnp.int32)
    table = members.reshape(top, rows).T
    table = table[jax.random.permutation(jax.random.fold_in(own, 1), rows)]
    rotation = jax.random.randint(jax.random.fold_in(own, 2), (rows, 1), 0, top)
    return jnp.take_along_axis(table, (jnp.arange(top)[None, :] + rotation) % top, axis=1)


def load_shares(amount, total, bound, slope, full):
    loads = [(1 << 20) // math.isqrt(rank ** slope) + 1 for rank in range(1, amount + 1)]
    largest = bound if full else min(bound, max(-(-total // amount), total * loads[0] // sum(loads)))
    least = 1 if total - largest >= amount - 1 else 0
    given, surplus = [largest] + [least] * (amount - 1), total - largest - least * (amount - 1)
    while surplus > 0:
        candidates = [i for i in range(1, amount) if given[i] < largest] or [i for i in range(1, amount) if given[i] < bound]
        whole, budget = sum([loads[i] for i in candidates]), surplus
        for i in candidates:
            addition = min(bound - given[i], max(1, budget * loads[i] // whole), surplus)
            given[i] = given[i] + addition
            surplus = surplus - addition
    return np.array(given)


def gaussian(own_key, extent, scale, reach, cuts=(), kind=jnp.bfloat16):
    loudness = level_of(own_key, extent, cuts, -0.22, 0.18) if cuts else 1.0
    entries = jax.random.normal(own_key, extent, jnp.float32) * scale * loudness
    return jnp.minimum(jnp.maximum(entries, -reach), reach).astype(kind)


def setup_inputs(seed: int = 0) -> dict:
    key_of = jax.random.split(jax.random.key(seed), 10)
    grad_out = gaussian(key_of[0], (TOKENS, D), 1.0, 6.0, ((0, 32),), jnp.float32)
    tokens = gaussian(key_of[1], (TOKENS, D), 1.0, 6.0, ((0, 32),))
    probs = jnp.clip(0.1 + 0.4 * jax.random.uniform(key_of[2], (TOKENS, TOP), jnp.float32) ** level_of(key_of[2], (TOKENS, TOP), ((0, 32),), -0.2, 0.2), 0.1, 0.5)
    expert_ids_keys = jax.random.split(jax.random.fold_in(key_of[3], 1), TOKENS // TOK_DEV)
    expert_ids_turns = jax.random.permutation(jax.random.fold_in(key_of[3], 3), TOKENS // TOK_DEV)
    expert_ids = jax.vmap(lambda own, number: deal_out(jax.random.fold_in(key_of[3], 2), own, number, TOK_DEV, EXPERTS, TOP, CAP, 2))(expert_ids_keys, expert_ids_turns).reshape((TOKENS, TOP))
    priority = jax.vmap(lambda own: jax.random.permutation(own, TOK_DEV))(jax.random.split(key_of[4], (N_EP * N_DP))).reshape((N_EP * N_DP, TOK_DEV)).astype(jnp.int32)
    cap_counts = draw_cap_counts(jax.random.fold_in(key_of[9], 71), 0)
    gate_weight = gaussian(key_of[6], (EXPERTS, FH, D), D ** -0.5, 0.15625, ((0, 8),))
    up_weight = gaussian(key_of[7], (EXPERTS, FH, D), D ** -0.5, 0.15625, ((0, 8),))
    down_weight = gaussian(key_of[8], (EXPERTS, FH, D), D ** -0.5, 0.15625, ((0, 8),))
    return dict(grad_out=grad_out, tokens=tokens, probs=probs, expert_ids=expert_ids, priority=priority, cap_counts=cap_counts, gate_weight=gate_weight, up_weight=up_weight, down_weight=down_weight)


sharpness = 1.702


def contract_last(first_op, second_op):
    return lax.dot_general(first_op, second_op, (((1,), (1,)), ((), ())), preferred_element_type=jnp.float32)


def replica_sum(deltas, values):
    per_replica = N_EP * CAP
    partials = jnp.einsum("rsf,rsd->rfd", deltas.reshape(N_DP, per_replica, FH).astype(jnp.float32), values.reshape(N_DP, per_replica, D).astype(jnp.float32), precision=lax.Precision.HIGHEST)
    rounded = lax.optimization_barrier(partials.astype(jnp.bfloat16))
    return jnp.sum(rounded.astype(jnp.float32), axis=0).astype(jnp.bfloat16)


def reference(grad_out, tokens, probs, expert_ids, priority, cap_counts, gate_weight, up_weight, down_weight):
    blocks = N_EP * N_DP
    slot_rows = N_EP * CAP
    total_slots = N_DP * slot_rows
    block_ids = expert_ids.reshape(blocks, TOK_DEV, TOP)
    expert_range = jnp.arange(EXPERTS, dtype=jnp.int32)
    routed = jnp.any(block_ids[:, :, :, None] == expert_range, axis=2).astype(jnp.float32)
    earlier = (priority[:, None, :] < priority[:, :, None]).astype(jnp.float32)
    before = jnp.einsum("bsu,bue->bse", earlier, routed, precision=lax.Precision.HIGHEST)
    slot_rank = jnp.take_along_axis(before, block_ids, axis=2).astype(jnp.int32)
    kept = slot_rank < cap_counts[block_ids]
    block_range = jnp.arange(blocks, dtype=jnp.int32)
    source = block_range // N_DP
    replica = block_range % N_DP
    position = (replica[:, None, None] * slot_rows + source[:, None, None] * CAP + slot_rank).reshape(TOKENS, TOP)
    kept = kept.reshape(TOKENS, TOP)
    row_scale = jnp.maximum(jnp.max(jnp.abs(grad_out), axis=1), 1.0)
    quantized = (grad_out / row_scale[:, None]).astype(jnp.bfloat16)

    def one_expert(running, inputs):
        input_acc, prob_acc = running
        expert, w_gate, w_up, w_down = inputs
        live_pair = kept & (expert_ids == expert)
        target = jnp.where(live_pair, position, total_slots).astype(jnp.int32)
        input_buf = jnp.zeros((total_slots + 1, D), jnp.bfloat16)
        grad_buf = jnp.zeros((total_slots + 1, D), jnp.bfloat16)
        scale_buf = jnp.zeros((total_slots + 1,), jnp.float32)
        prob_buf = jnp.zeros((total_slots + 1,), jnp.float32)
        for which in range(TOP):
            input_buf = input_buf.at[target[:, which]].set(tokens)
            grad_buf = grad_buf.at[target[:, which]].set(quantized)
            scale_buf = scale_buf.at[target[:, which]].set(row_scale)
            prob_buf = prob_buf.at[target[:, which]].set(probs[:, which])
        slot_x = input_buf[:total_slots]
        slot_q = grad_buf[:total_slots]
        slot_scale = scale_buf[:total_slots]
        slot_prob = prob_buf[:total_slots]
        gate_pre = contract_last(slot_x, w_gate)
        up_pre = contract_last(slot_x, w_up)
        back_proj = contract_last(slot_q, w_down)
        squash = jax.nn.sigmoid(sharpness * gate_pre)
        gated = gate_pre * squash
        activated = (up_pre + 1.0) * gated
        weight = (slot_scale * slot_prob)[:, None]
        act_delta = weight * back_proj
        up_delta = (act_delta * gated).astype(jnp.bfloat16)
        gate_delta = (act_delta * (up_pre + 1.0) * (squash + sharpness * gate_pre * squash * (1.0 - squash))).astype(jnp.bfloat16)
        act_scaled = (activated * weight).astype(jnp.bfloat16)
        slot_in = (jnp.dot(gate_delta, w_gate, preferred_element_type=jnp.float32) + jnp.dot(up_delta, w_up, preferred_element_type=jnp.float32)).astype(jnp.bfloat16)
        slot_pgrad = slot_scale * jnp.sum(activated * back_proj, axis=1)
        pad_in = jnp.concatenate([slot_in, jnp.zeros((1, D), jnp.bfloat16)], axis=0)
        pad_prob = jnp.concatenate([slot_pgrad, jnp.zeros((1,), jnp.float32)], axis=0)
        for which in range(TOP):
            input_acc = input_acc + pad_in[target[:, which]].astype(jnp.float32)
        prob_acc = prob_acc + pad_prob[target]
        grads = (replica_sum(gate_delta, slot_x), replica_sum(up_delta, slot_x), replica_sum(act_scaled, slot_q))
        return (input_acc, prob_acc), grads

    start = (jnp.zeros((TOKENS, D), jnp.float32), jnp.zeros((TOKENS, TOP), jnp.float32))
    (input_acc, prob_acc), grads = lax.scan(one_expert, start, (expert_range, gate_weight, up_weight, down_weight))
    return input_acc.astype(jnp.bfloat16), prob_acc, grads[0], grads[1], grads[2]
```

```python
import jax
import jax.numpy as jnp
from jax import lax
from jax.sharding import PartitionSpec as P

highest = lax.Precision.HIGHEST
sharpness = 1.702
lanes = 128


def contract_last(first_op, second_op):
    return lax.dot_general(
        first_op, second_op, (((1,), (1,)), ((), ())), preferred_element_type=jnp.float32
    )


def contract_first(first_op, second_op):
    return lax.dot_general(
        first_op, second_op, (((0,), (0,)), ((), ())), preferred_element_type=jnp.float32
    )


def high_low(values):
    high = lax.reduce_precision(values, 8, 7)
    return high, values - high


def slot_positions(expert_ids, priority, cap_counts, buckets, capacity):
    ranking = priority[0]
    earlier = (ranking[None, :] < ranking[:, None]).astype(jnp.bfloat16)
    expert_range = lax.broadcasted_iota(jnp.int32, (1, 1, buckets), 2)
    matches = (expert_ids[:, :, None] == expert_range).astype(jnp.float32)
    routed = jnp.sum(matches, axis=1).astype(jnp.bfloat16)
    before = jnp.dot(earlier, routed, preferred_element_type=jnp.float32)
    slot_rank = jnp.sum(matches * before[:, None, :], axis=2)
    keep_limit = jnp.sum(matches * cap_counts.astype(jnp.float32)[None, None, :], axis=2)
    position = expert_ids * capacity + slot_rank.astype(jnp.int32)
    return jnp.where(slot_rank < keep_limit, position, -1)


def activation(gate_pre, up_pre):
    squash = jax.nn.sigmoid(sharpness * gate_pre)
    gated = gate_pre * squash
    return squash, gated, (up_pre + 1.0) * gated


def deltas(gate_pre, up_pre, back_proj, weight):
    squash, gated, activated = activation(gate_pre, up_pre)
    act_delta = weight * back_proj
    up_delta = (act_delta * gated).astype(jnp.bfloat16)
    gate_delta = (
        act_delta * (up_pre + 1.0) * (squash + sharpness * gate_pre * squash * (1.0 - squash))
    ).astype(jnp.bfloat16)
    return activated, gate_delta, up_delta


def on_device(
    grad_out, tokens, probs, expert_ids, priority, cap_counts, gate_weight, up_weight, down_weight
):
    ep_size = lax.axis_size("ep")
    dp_size = lax.axis_size("dp")
    ep_rank = lax.axis_index("ep")
    dp_rank = lax.axis_index("dp")
    tok_rows, model_width = tokens.shape
    route_count = expert_ids.shape[1]
    hidden = gate_weight.shape[1]
    quarter = hidden // dp_size
    capacity = 5 * route_count * tok_rows // (4 * ep_size)
    slot_rows = ep_size * capacity
    wide = model_width + lanes

    position = slot_positions(expert_ids, priority, cap_counts, ep_size, capacity)
    slot_range = lax.broadcasted_iota(jnp.int32, (1, 1, slot_rows), 2)
    placement = (position[:, :, None] == slot_range).astype(jnp.bfloat16)
    table = jnp.sum(placement, axis=1)

    row_scale = jnp.maximum(jnp.max(jnp.abs(grad_out), axis=1), 1.0)
    quantized = (grad_out / row_scale[:, None]).astype(jnp.bfloat16)
    scale_parts = high_low(row_scale[:, None])
    prob_parts = high_low(probs)
    facts = jnp.concatenate(
        [*prob_parts, expert_ids.astype(jnp.float32), *scale_parts], axis=1
    ).astype(jnp.bfloat16)
    facts = jnp.pad(facts, ((0, 0), (0, lanes - facts.shape[1])))
    payload = jnp.concatenate([tokens, facts], axis=1)

    def to_slots(rows):
        return contract_first(table, rows).astype(jnp.bfloat16)

    def exchange(rows):
        width = rows.shape[-1]
        return lax.all_to_all(
            rows.reshape(ep_size, capacity, width), "ep", split_axis=0, concat_axis=0, tiled=True
        ).reshape(slot_rows, width)

    def gather_replicas(rows):
        blocks = [rows]
        step = dp_size // 2
        while step:
            swap = [(d, d ^ step) for d in range(dp_size)]
            blocks += [lax.ppermute(block, "dp", swap) for block in blocks]
            step //= 2
        return blocks

    own_x = exchange(to_slots(payload))
    own_x, quantized = lax.optimization_barrier((own_x, quantized))
    blocks_x = gather_replicas(own_x)
    own_q = exchange(to_slots(quantized))
    blocks_q = gather_replicas(own_q)

    w_gate = gate_weight[0]
    w_up = up_weight[0]
    w_down = down_weight[0]

    def slot_facts(block):
        values = block[:, model_width:].astype(jnp.float32)
        k = route_count
        pair_probs = values[:, :k] + values[:, k : 2 * k]
        mine = values[:, 2 * k : 3 * k] == ep_rank.astype(jnp.float32)
        prob = jnp.sum(jnp.where(mine, pair_probs, 0.0), axis=1, keepdims=True)
        scale = values[:, 3 * k : 3 * k + 1] + values[:, 3 * k + 1 : 3 * k + 2]
        return scale, scale * prob

    slot_x = own_x[:, :model_width]
    scale, weight = slot_facts(own_x)
    back_proj = contract_last(own_q, w_down)
    activated, gate_delta, up_delta = deltas(
        contract_last(slot_x, w_gate), contract_last(slot_x, w_up), back_proj, weight
    )
    slot_in = (
        jnp.dot(gate_delta, w_gate, preferred_element_type=jnp.float32)
        + jnp.dot(up_delta, w_up, preferred_element_type=jnp.float32)
    ).astype(jnp.bfloat16)
    slot_pgrad = scale * jnp.sum(activated * back_proj, axis=1, keepdims=True)
    pgrad_parts = jnp.concatenate(high_low(slot_pgrad), axis=1).astype(jnp.bfloat16)
    pgrad_parts = jnp.pad(pgrad_parts, ((0, 0), (0, lanes - 2)))
    back = exchange(jnp.concatenate([slot_in, pgrad_parts], axis=1))

    def own_units(matrix):
        return lax.dynamic_slice_in_dim(matrix, dp_rank * quarter, quarter, axis=0)

    q_gate, q_up, q_down = own_units(w_gate), own_units(w_up), own_units(w_down)
    sums = None
    for block_x, block_q in zip(blocks_x, blocks_q):
        rows = block_x[:, :model_width]
        _, block_weight = slot_facts(block_x)
        act, g_delta, u_delta = deltas(
            contract_last(rows, q_gate),
            contract_last(rows, q_up),
            contract_last(block_q, q_down),
            block_weight,
        )
        act_scaled = (act * block_weight).astype(jnp.bfloat16)
        parts = (
            contract_first(g_delta, rows),
            contract_first(u_delta, rows),
            contract_first(act_scaled, block_q),
        )
        sums = parts if sums is None else tuple(a + b for a, b in zip(sums, parts))
    gate_share, up_share, down_share = (s.astype(jnp.bfloat16) for s in sums)

    input_grad = jnp.dot(
        table, back[:, :model_width], preferred_element_type=jnp.float32
    ).astype(jnp.bfloat16)
    pair_rows = placement.reshape(tok_rows * route_count, slot_rows)
    pair_grad = jnp.dot(pair_rows, back[:, model_width:], preferred_element_type=jnp.float32)
    prob_grad = (pair_grad[:, 0] + pair_grad[:, 1]).reshape(tok_rows, route_count)
    return (input_grad, prob_grad, gate_share[None], up_share[None], down_share[None])


def solution(mesh):
    return jax.shard_map(
        on_device,
        mesh=mesh,
        in_specs=(
            P(("ep", "dp"), None),
            P(("ep", "dp"), None),
            P(("ep", "dp"), None),
            P(("ep", "dp"), None),
            P(("ep", "dp"), None),
            P(),
            P("ep", None, None),
            P("ep", None, None),
            P("ep", None, None),
        ),
        out_specs=(
            P(("ep", "dp"), None),
            P(("ep", "dp"), None),
            P("ep", "dp", None),
            P("ep", "dp", None),
            P("ep", "dp", None),
        ),
        check_vma=False,
    )
```

```python
import functools

import jax
import jax.numpy as jnp
from jax import lax
from jax.experimental import pallas as pl
from jax.experimental.pallas import tpu as pltpu
from jax.sharding import PartitionSpec as P

sharpness = 1.702
lanes = 128

params = functools.partial(pltpu.CompilerParams, vmem_limit_bytes=56 * 1024 * 1024)


def contract_last(first_op, second_op):
    return lax.dot_general(
        first_op, second_op, (((1,), (1,)), ((), ())), preferred_element_type=jnp.float32
    )


def contract_first(first_op, second_op):
    return lax.dot_general(
        first_op, second_op, (((0,), (0,)), ((), ())), preferred_element_type=jnp.float32
    )


def high_low(values):
    high = values.astype(jnp.bfloat16)
    return high, (values - high.astype(jnp.float32)).astype(jnp.bfloat16)


def iota(shape, dim):
    return lax.broadcasted_iota(jnp.int32, shape, dim)


def lane_sum(values, first, stop):
    lane = iota(values.shape, 1)
    return jnp.sum(jnp.where((lane >= first) & (lane < stop), values, 0.0), axis=1, keepdims=True)


def prep_kernel(cap_ref, ids_ref, order_ref, probs_ref, grad_ref, tok_ref, x_ref, q_ref, pos_ref,
                *, experts, capacity):
    rows, width = tok_ref.shape
    routes = ids_ref.shape[1]
    slots = experts * capacity
    lane = iota((rows, lanes), 1)
    order = order_ref[...].astype(jnp.float32)
    across = jnp.broadcast_to(order, (rows, rows))
    earlier = (across < across.T).astype(jnp.bfloat16)
    ids = [ids_ref[:, k : k + 1] for k in range(routes)]
    hits = [lane == i for i in ids]
    routed = sum(h.astype(jnp.float32) for h in hits)
    before = jnp.dot(earlier, routed.astype(jnp.bfloat16), preferred_element_type=jnp.float32)
    limit = jnp.zeros((1, lanes), jnp.float32)
    for e in range(experts):
        limit = jnp.where(lane[:1] == e, cap_ref[e].astype(jnp.float32), limit)
    slot = iota((rows, slots), 1)
    position = jnp.full((rows, lanes), -1, jnp.int32)
    table = jnp.zeros((rows, slots), jnp.float32)
    chance = jnp.zeros((rows, slots), jnp.float32)
    for k in range(routes):
        rank = jnp.sum(jnp.where(hits[k], before, 0.0), axis=1, keepdims=True)
        most = jnp.sum(
            jnp.where(hits[k], jnp.broadcast_to(limit, (rows, lanes)), 0.0), axis=1, keepdims=True
        )
        place = jnp.where(rank < most, ids[k] * capacity + rank.astype(jnp.int32), -1)
        position = jnp.where(lane == k, place, position)
        hit = (slot == place).astype(jnp.float32)
        table = table + hit
        chance = chance + hit * probs_ref[:, k : k + 1]
    pos_ref[...] = position
    table = table.astype(jnp.bfloat16)
    x_ref[:, :width] = contract_first(table, tok_ref[...]).astype(jnp.bfloat16)
    grad = grad_ref[...]
    scale = jnp.maximum(jnp.max(jnp.abs(grad), axis=1, keepdims=True), 1.0)
    quantized = (grad / scale).astype(jnp.bfloat16)
    q_ref[...] = contract_first(table, quantized).astype(jnp.bfloat16)
    chance_high, chance_low = high_low(chance)
    scale_high, scale_low = (s.astype(jnp.float32) for s in high_low(scale))
    scales = jnp.where(lane == 2, scale_high, jnp.where(lane == 3, scale_low, 0.0))
    facts = (
        contract_first(chance_high, (lane == 0).astype(jnp.bfloat16))
        + contract_first(chance_low, (lane == 1).astype(jnp.bfloat16))
        + contract_first(table, scales.astype(jnp.bfloat16))
    )
    x_ref[:, width:] = facts.astype(jnp.bfloat16)


def slot_facts(values):
    values = values.astype(jnp.float32)
    scale = lane_sum(values, 2, 4)
    return scale, scale * lane_sum(values, 0, 2)


def x_kernel(rank_ref, x_ref, gate_ref, up_ref, gated_ref, slope_ref, act_ref):
    del rank_ref
    width = gate_ref.shape[1]
    x = x_ref[:, :width]
    gate_pre = contract_last(x, gate_ref[...])
    up_pre = contract_last(x, up_ref[...])
    squash = jax.nn.sigmoid(sharpness * gate_pre)
    gated = gate_pre * squash
    more = up_pre + 1.0
    gated_ref[0] = gated.astype(jnp.bfloat16)
    slope_ref[0] = (more * (squash + sharpness * gated * (1.0 - squash))).astype(jnp.bfloat16)
    act_ref[0] = (more * gated).astype(jnp.bfloat16)


def q_kernel(rank_ref, q_ref, facts_ref, gate_ref, up_ref, down_ref, gated_ref, slope_ref, act_ref,
             out_ref, sum_ref, prob_ref):
    del rank_ref
    step = pl.program_id(0)
    width = q_ref.shape[1]
    scale, weight = slot_facts(facts_ref[...])
    back_proj = contract_last(q_ref[...], down_ref[...])
    delta = weight * back_proj
    up_delta = (delta * gated_ref[0].astype(jnp.float32)).astype(jnp.bfloat16)
    gate_delta = (delta * slope_ref[0].astype(jnp.float32)).astype(jnp.bfloat16)
    share = jnp.dot(gate_delta, gate_ref[...], preferred_element_type=jnp.float32) + jnp.dot(
        up_delta, up_ref[...], preferred_element_type=jnp.float32
    )
    term = jnp.sum(act_ref[0].astype(jnp.float32) * back_proj, axis=1, keepdims=True)

    @pl.when(step == 0)
    def _():
        sum_ref[...] = share
        prob_ref[...] = term

    @pl.when(step > 0)
    def _():
        sum_ref[...] += share
        prob_ref[...] += term

    @pl.when(step == pl.num_programs(0) - 1)
    def _():
        out_ref[:, :width] = sum_ref[...].astype(jnp.bfloat16)
        high, low = high_low(scale * prob_ref[...])
        lane = iota((out_ref.shape[0], lanes), 1)
        out_ref[:, width:] = jnp.where(
            lane == 0, high.astype(jnp.float32), jnp.where(lane == 1, low.astype(jnp.float32), 0.0)
        ).astype(jnp.bfloat16)


def weight_kernel(rank_ref, *refs, blocks, rows, with_start):
    x_hbm, q_hbm, gated_hbm, slope_hbm, act_hbm = (
        refs[i * blocks : (i + 1) * blocks] for i in range(5)
    )
    refs = refs[5 * blocks :]
    down_hbm, refs = refs[0], refs[1:]
    starts, refs = (refs[:3], refs[3:]) if with_start else ((), refs)
    outs, refs = refs[:3], refs[3:]
    x, q, gated, slope, act, down = refs[:6]
    held = refs[6:9] if with_start else ()
    sems = refs[-1]
    copies = []

    def fetch(source, target):
        copy = pltpu.make_async_copy(source, target, sems.at[len(copies)])
        copy.start()
        copies.append(copy)
        return copy

    quarter = down.shape[0]
    first = [fetch(down_hbm.at[pl.ds(rank_ref[0] * quarter, quarter), :], down)]
    for b in range(blocks):
        first.append(fetch(q_hbm[b], q.at[pl.ds(b * rows, rows)]))
    second = []
    for b in range(blocks):
        part = pl.ds(b * rows, rows)
        second += [
            fetch(gated_hbm[b].at[0], gated.at[part]),
            fetch(slope_hbm[b].at[0], slope.at[part]),
            fetch(act_hbm[b].at[0], act.at[part]),
            fetch(x_hbm[b], x.at[part]),
        ]
    third = [fetch(s, h) for s, h in zip(starts, held)]
    for copy in first:
        copy.wait()
    back_proj = contract_last(q[...], down[...])
    for copy in second:
        copy.wait()
    width = q.shape[1]
    _, weight = slot_facts(x[:, width:])
    delta = weight * back_proj
    up_delta = (delta * gated[...].astype(jnp.float32)).astype(jnp.bfloat16)
    gate_delta = (delta * slope[...].astype(jnp.float32)).astype(jnp.bfloat16)
    act_scaled = (act[...].astype(jnp.float32) * weight).astype(jnp.bfloat16)
    rows_x = x[:, :width]
    for copy in third:
        copy.wait()
    for i, (left, right) in enumerate(
        ((gate_delta, rows_x), (up_delta, rows_x), (act_scaled, q[...]))
    ):
        total = contract_first(left, right)
        if with_start:
            total = total + held[i][...]
        outs[i][...] = total.astype(outs[i].dtype)


def combine_kernel(pos_ref, back_ref, grad_ref, prob_ref):
    rows = pos_ref.shape[0]
    slots, wide = back_ref.shape
    width = wide - lanes
    routes = prob_ref.shape[1]
    slot = iota((rows, slots), 1)
    table = jnp.zeros((rows, slots), jnp.float32)
    for k in range(routes):
        hit = (slot == pos_ref[:, k : k + 1]).astype(jnp.float32)
        table = table + hit
        pairs = jnp.dot(
            hit.astype(jnp.bfloat16), back_ref[:, width:], preferred_element_type=jnp.float32
        )
        prob_ref[:, k : k + 1] = lane_sum(pairs, 0, 2)
    grad_ref[...] = jnp.dot(
        table.astype(jnp.bfloat16), back_ref[:, :width], preferred_element_type=jnp.float32
    ).astype(jnp.bfloat16)


def on_device(
    grad_out, tokens, probs, expert_ids, priority, cap_counts, gate_weight, up_weight, down_weight
):
    ep_size = lax.axis_size("ep")
    dp_size = lax.axis_size("dp")
    rank = lax.axis_index("dp").reshape(1).astype(jnp.int32)
    tok_rows, model_width = tokens.shape
    route_count = expert_ids.shape[1]
    hidden = gate_weight.shape[1]
    quarter = hidden // dp_size
    capacity = 5 * route_count * tok_rows // (4 * ep_size)
    slots = ep_size * capacity
    wide = model_width + lanes
    w_gate, w_up, w_down = gate_weight[0], up_weight[0], down_weight[0]
    bf16, f32 = jnp.bfloat16, jnp.float32
    shape = jax.ShapeDtypeStruct
    vmem = pl.BlockSpec(memory_space=pltpu.VMEM)
    smem = pl.BlockSpec(memory_space=pltpu.SMEM)
    hbm = pl.BlockSpec(memory_space=pltpu.HBM)

    send_x, send_q, position = pl.pallas_call(
        functools.partial(prep_kernel, experts=ep_size, capacity=capacity),
        out_shape=(
            shape((slots, wide), bf16),
            shape((slots, model_width), bf16),
            shape((tok_rows, lanes), jnp.int32),
        ),
        in_specs=[smem] + [vmem] * 5,
        out_specs=(vmem,) * 3,
        compiler_params=params(),
        name="prep",
    )(cap_counts, expert_ids, priority, probs, grad_out, tokens)

    def exchange(rows):
        width = rows.shape[-1]
        return lax.all_to_all(
            rows.reshape(ep_size, capacity, width), "ep", split_axis=0, concat_axis=0, tiled=True
        ).reshape(slots, width)

    def swap(rows, step):
        return lax.ppermute(rows, "dp", [(d, d ^ step) for d in range(dp_size)])

    def gather_replicas(rows):
        near = [rows]
        far = [swap(rows, dp_size // 2)]
        step = dp_size // 4
        while step:
            near += [swap(block, step) for block in near]
            far += [swap(block, step) for block in far]
            step //= 2
        return near, far

    def x_part(rows, tiles):
        turn = lambda j, r: ((r[0] + j) % dp_size, 0)
        out = pl.BlockSpec((1, slots, quarter), lambda j, r: (j, 0, 0))
        return pl.pallas_call(
            x_kernel,
            grid_spec=pltpu.PrefetchScalarGridSpec(
                num_scalar_prefetch=1,
                grid=(tiles,),
                in_specs=[
                    pl.BlockSpec((slots, wide), lambda j, r: (0, 0)),
                    pl.BlockSpec((quarter, model_width), turn),
                    pl.BlockSpec((quarter, model_width), turn),
                ],
                out_specs=(out,) * 3,
            ),
            out_shape=(shape((tiles, slots, quarter), bf16),) * 3,
            compiler_params=params(),
            cost_estimate=pl.CostEstimate(
                flops=4 * slots * model_width * quarter * tiles,
                bytes_accessed=2 * slots * wide + 4 * tiles * quarter * model_width,
                transcendentals=tiles * slots * quarter,
            ),
            name="x_part",
        )(rank, rows, w_gate, w_up)

    def q_part(rows_q, rows_x, parts):
        turn = lambda j, r: ((r[0] + j) % dp_size, 0)
        tile = pl.BlockSpec((1, slots, quarter), lambda j, r: (j, 0, 0))
        return pl.pallas_call(
            q_kernel,
            grid_spec=pltpu.PrefetchScalarGridSpec(
                num_scalar_prefetch=1,
                grid=(dp_size,),
                in_specs=[
                    pl.BlockSpec((slots, model_width), lambda j, r: (0, 0)),
                    pl.BlockSpec((slots, lanes), lambda j, r: (0, model_width // lanes)),
                    pl.BlockSpec((quarter, model_width), turn),
                    pl.BlockSpec((quarter, model_width), turn),
                    pl.BlockSpec((quarter, model_width), turn),
                    tile,
                    tile,
                    tile,
                ],
                out_specs=pl.BlockSpec((slots, wide), lambda j, r: (0, 0)),
                scratch_shapes=[
                    pltpu.VMEM((slots, model_width), f32),
                    pltpu.VMEM((slots, 1), f32),
                ],
            ),
            out_shape=shape((slots, wide), bf16),
            compiler_params=params(),
            cost_estimate=pl.CostEstimate(
                flops=6 * slots * model_width * hidden,
                bytes_accessed=6 * hidden * model_width,
                transcendentals=0,
            ),
            name="q_part",
        )(rank, rows_q, rows_x, w_gate, w_up, w_down, *parts)

    def weight_grads(blocks_x, blocks_q, parts, start, out_type):
        count = len(blocks_x)
        rows = count * slots
        columns = list(zip(*parts))
        operands = [*blocks_x, *blocks_q, *columns[0], *columns[1], *columns[2], w_down]
        operands += list(start or ())
        scratch = [pltpu.VMEM((rows, wide), bf16), pltpu.VMEM((rows, model_width), bf16)]
        scratch += [pltpu.VMEM((rows, quarter), bf16)] * 3
        scratch += [pltpu.VMEM((quarter, model_width), bf16)]
        if start:
            scratch += [pltpu.VMEM((quarter, model_width), f32)] * 3
        scratch += [pltpu.SemaphoreType.DMA((len(operands),))]
        return pl.pallas_call(
            functools.partial(
                weight_kernel, blocks=count, rows=slots, with_start=start is not None
            ),
            out_shape=(shape((quarter, model_width), out_type),) * 3,
            in_specs=[smem] + [hbm] * len(operands),
            out_specs=(vmem,) * 3,
            scratch_shapes=scratch,
            compiler_params=params(),
            cost_estimate=pl.CostEstimate(
                flops=8 * rows * model_width * quarter,
                bytes_accessed=4 * rows * wide,
                transcendentals=0,
            ),
            name="weight_grads",
        )(rank, *operands)

    own_x = exchange(send_x)
    own_x, send_q = lax.optimization_barrier((own_x, send_q))
    own_q = exchange(send_q)
    near_x, far_x = gather_replicas(own_x)
    near_q, far_q = gather_replicas(own_q)
    own_parts = x_part(own_x, dp_size)
    near_parts = [own_parts] + [x_part(block, 1) for block in near_x[1:]]
    far_parts = [x_part(block, 1) for block in far_x]
    back = exchange(q_part(own_q, own_x, own_parts))
    near_sums = weight_grads(near_x, near_q, near_parts, None, f32)
    shares = weight_grads(far_x, far_q, far_parts, near_sums, bf16)
    input_grad, prob_grad = pl.pallas_call(
        combine_kernel,
        out_shape=(shape((tok_rows, model_width), bf16), shape((tok_rows, route_count), f32)),
        in_specs=[vmem] * 2,
        out_specs=(vmem,) * 2,
        compiler_params=params(),
        name="combine",
    )(position, back)
    return (input_grad, prob_grad, *(share[None] for share in shares))


def solution(mesh):
    return jax.shard_map(
        on_device,
        mesh=mesh,
        in_specs=(
            P(("ep", "dp"), None),
            P(("ep", "dp"), None),
            P(("ep", "dp"), None),
            P(("ep", "dp"), None),
            P(("ep", "dp"), None),
            P(),
            P("ep", None, None),
            P("ep", None, None),
            P("ep", None, None),
        ),
        out_specs=(
            P(("ep", "dp"), None),
            P(("ep", "dp"), None),
            P("ep", "dp", None),
            P("ep", "dp", None),
            P("ep", "dp", None),
        ),
        check_vma=False,
    )
```

```python
import functools

import jax
import jax.numpy as jnp
from jax import lax
from jax.experimental import pallas as pl
from jax.experimental.pallas import tpu as pltpu
from jax.sharding import PartitionSpec as P


sharpness = 1.702
lanes = 128

params = functools.partial(pltpu.CompilerParams, vmem_limit_bytes=56 * 1024 * 1024)


def contract_last(first_op, second_op):
    return lax.dot_general(
        first_op, second_op, (((1,), (1,)), ((), ())), preferred_element_type=jnp.float32
    )


def contract_first(first_op, second_op):
    return lax.dot_general(
        first_op, second_op, (((0,), (0,)), ((), ())), preferred_element_type=jnp.float32
    )


def high_low(values):
    high = values.astype(jnp.bfloat16)
    return high, (values - high.astype(jnp.float32)).astype(jnp.bfloat16)


def iota(shape, dim):
    return lax.broadcasted_iota(jnp.int32, shape, dim)


def lane_sum(values, first, stop):
    lane = iota(values.shape, 1)
    return jnp.sum(jnp.where((lane >= first) & (lane < stop), values, 0.0), axis=1, keepdims=True)


def columns_of(rows_ref, count):
    n = rows_ref.shape[1]
    return [
        jnp.broadcast_to(rows_ref[k : k + 1, :].astype(jnp.float32), (n, n)).T
        for k in range(count)
    ]


def prep_kernel(cap_ref, ids_ref, order_ref, probs_ref, grad_ref, tok_ref, x_ref, q_ref, *, experts):
    rows, width = tok_ref.shape
    routes = ids_ref.shape[0]
    lane = iota((rows, lanes), 1)
    lane_f = lane.astype(jnp.float32)
    order = jnp.broadcast_to(order_ref[...].astype(jnp.float32), (rows, rows))
    earlier = (order < order.T).astype(jnp.bfloat16)
    ids = columns_of(ids_ref, routes)
    chances = columns_of(probs_ref, routes)
    hits = [lane_f == i for i in ids]
    routed = sum(h.astype(jnp.float32) for h in hits)
    before = jnp.dot(earlier, routed.astype(jnp.bfloat16), preferred_element_type=jnp.float32)
    limit = jnp.zeros((rows, lanes), jnp.float32)
    for e in range(experts):
        limit = jnp.where(lane == e, cap_ref[e].astype(jnp.float32), limit)
    grad = grad_ref[...]
    scale = jnp.maximum(jnp.max(jnp.abs(grad), axis=1, keepdims=True), 1.0)
    q_ref[...] = (grad / scale).astype(jnp.bfloat16)
    facts = jnp.zeros((rows, lanes), jnp.float32)
    for k in range(routes):
        rank = jnp.sum(jnp.where(hits[k], before, 0.0), axis=1, keepdims=True)
        most = jnp.sum(jnp.where(hits[k], limit, 0.0), axis=1, keepdims=True)
        high, low = (p.astype(jnp.float32) for p in high_low(chances[k]))
        facts = jnp.where(lane == k, ids[k], facts)
        facts = jnp.where(lane == routes + k, jnp.where(rank < most, rank, -1.0), facts)
        facts = jnp.where(lane == 2 * routes + k, high, facts)
        facts = jnp.where(lane == 3 * routes + k, low, facts)
    high, low = (s.astype(jnp.float32) for s in high_low(scale))
    facts = jnp.where(lane == 4 * routes, high, facts)
    facts = jnp.where(lane == 4 * routes + 1, low, facts)
    x_ref[:, :width] = tok_ref[...]
    x_ref[:, width:] = facts.astype(jnp.bfloat16)


def chunks_of(place_ref, refs, outer, inner):
    if len(refs) == outer:
        return jnp.concatenate([r[...] for r in refs], axis=0)
    own, below, above, down, up, across = refs
    z = lax.div(place_ref[0], inner)
    back = jnp.where(z == 0, across[...], below[...])
    ahead = jnp.where(z == outer - 1, across[...], above[...])
    middle = jnp.where(z < outer // 2, down[...], up[...])
    return jnp.concatenate([own[...], back, middle, ahead], axis=0)


def partner(ep_rank, steps, places, outer, inner):
    z = lax.rem(lax.div(ep_rank, inner) + steps, outer)
    return (z * inner + lax.rem(lax.rem(ep_rank, inner) + places, inner)).astype(jnp.float32)


def x_slots_kernel(place_ref, *refs, outer, inner, capacity, routes):
    outs = refs[-inner - 1 :]
    rows = chunks_of(place_ref, refs[: -inner - 1], outer, inner)
    count, wide = rows.shape
    width = wide - lanes
    block = outer * capacity
    facts = rows[:, width:].astype(jnp.float32)
    chunk = (iota((count, 1), 0) // (count // outer)).astype(jnp.float32)
    slot = iota((count, inner * block), 1).astype(jnp.float32)
    table = jnp.zeros((count, inner * block), jnp.float32)
    chance = jnp.zeros((count, inner * block), jnp.float32)
    for k in range(routes):
        expert = facts[:, k : k + 1]
        rank = facts[:, routes + k : routes + k + 1]
        prob = facts[:, 2 * routes + k : 2 * routes + k + 1]
        prob = prob + facts[:, 3 * routes + k : 3 * routes + k + 1]
        column = jnp.full((count, 1), -1.0, jnp.float32)
        for d in range(inner):
            mine = (expert == partner(place_ref[0], 0, d, outer, inner)) & (rank >= 0.0)
            column = jnp.where(mine, d * block + chunk * capacity + rank, column)
        hit = (slot == column).astype(jnp.float32)
        table = table + hit
        chance = chance + hit * prob
    table = table.astype(jnp.bfloat16)
    outs[-1][...] = table
    chance_high, chance_low = high_low(chance)
    lane = iota((count, lanes), 1)
    scales = jnp.where(
        lane == 2,
        facts[:, 4 * routes : 4 * routes + 1],
        jnp.where(lane == 3, facts[:, 4 * routes + 1 : 4 * routes + 2], 0.0),
    ).astype(jnp.bfloat16)
    kept = (
        contract_first(chance_high, (lane == 0).astype(jnp.bfloat16))
        + contract_first(chance_low, (lane == 1).astype(jnp.bfloat16))
        + contract_first(table, scales)
    ).astype(jnp.bfloat16)
    for d in range(inner):
        part = slice(d * block, (d + 1) * block)
        outs[d][:, :width] = contract_first(table[:, part], rows[:, :width]).astype(jnp.bfloat16)
        outs[d][:, width:] = kept[part]


def q_slots_kernel(place_ref, table_ref, *refs, outer, inner):
    outs = refs[-inner:]
    rows = chunks_of(place_ref, refs[:-inner], outer, inner)
    block = table_ref.shape[1] // inner
    for d in range(inner):
        part = table_ref[:, d * block : (d + 1) * block]
        outs[d][...] = contract_first(part, rows).astype(jnp.bfloat16)


def slot_facts(values):
    values = values.astype(jnp.float32)
    scale = lane_sum(values, 2, 4)
    return scale, scale * lane_sum(values, 0, 2)


def x_kernel(rank_ref, x_ref, gate_ref, up_ref, gated_ref, slope_ref, act_ref):
    del rank_ref
    width = gate_ref.shape[1]
    x = x_ref[:, :width]
    gate_pre = contract_last(x, gate_ref[...])
    up_pre = contract_last(x, up_ref[...])
    squash = jax.nn.sigmoid(sharpness * gate_pre)
    gated = gate_pre * squash
    more = up_pre + 1.0
    gated_ref[0] = gated.astype(jnp.bfloat16)
    slope_ref[0] = (more * (squash + sharpness * gated * (1.0 - squash))).astype(jnp.bfloat16)
    act_ref[0] = (more * gated).astype(jnp.bfloat16)


def q_kernel(rank_ref, q_ref, facts_ref, gate_ref, up_ref, down_ref, gated_ref, slope_ref, act_ref,
             out_ref, sum_ref, prob_ref):
    del rank_ref
    step = pl.program_id(0)
    width = q_ref.shape[1]
    scale, weight = slot_facts(facts_ref[...])
    back_proj = contract_last(q_ref[...], down_ref[...])
    delta = weight * back_proj
    up_delta = (delta * gated_ref[0].astype(jnp.float32)).astype(jnp.bfloat16)
    gate_delta = (delta * slope_ref[0].astype(jnp.float32)).astype(jnp.bfloat16)
    share = jnp.dot(gate_delta, gate_ref[...], preferred_element_type=jnp.float32) + jnp.dot(
        up_delta, up_ref[...], preferred_element_type=jnp.float32
    )
    term = jnp.sum(act_ref[0].astype(jnp.float32) * back_proj, axis=1, keepdims=True)

    @pl.when(step == 0)
    def _():
        sum_ref[...] = share
        prob_ref[...] = term

    @pl.when(step > 0)
    def _():
        sum_ref[...] += share
        prob_ref[...] += term

    @pl.when(step == pl.num_programs(0) - 1)
    def _():
        out_ref[:, :width] = sum_ref[...].astype(jnp.bfloat16)
        high, low = high_low(scale * prob_ref[...])
        lane = iota((out_ref.shape[0], lanes), 1)
        out_ref[:, width:] = jnp.where(
            lane == 0, high.astype(jnp.float32), jnp.where(lane == 1, low.astype(jnp.float32), 0.0)
        ).astype(jnp.bfloat16)


def weight_kernel(rank_ref, *refs, blocks, rows, with_start):
    x_hbm, refs = refs[:blocks], refs[blocks:]
    q_hbm, refs = refs[:blocks], refs[blocks:]
    weights_hbm, refs = refs[:3], refs[3:]
    starts, refs = (refs[:3], refs[3:]) if with_start else ((), refs)
    outs, refs = refs[:3], refs[3:]
    x, q, refs = refs[0], refs[1], refs[2:]
    weights, refs = refs[:3], refs[3:]
    held = refs[:3] if with_start else ()
    sems = refs[-1]
    copies = []

    def fetch(source, target):
        copy = pltpu.make_async_copy(source, target, sems.at[len(copies)])
        copy.start()
        copies.append(copy)
        return copy

    quarter = weights[0].shape[0]
    mine = pl.ds(rank_ref[0] * quarter, quarter)
    first = [fetch(w.at[mine, :], v) for w, v in zip(weights_hbm, weights)]
    first += [fetch(x_hbm[b], x.at[pl.ds(b * rows, rows)]) for b in range(blocks)]
    second = [fetch(q_hbm[b], q.at[pl.ds(b * rows, rows)]) for b in range(blocks)]
    third = [fetch(s, h) for s, h in zip(starts, held)]
    for copy in first:
        copy.wait()
    width = q.shape[1]
    gate_pre = contract_last(x[:, :width], weights[0][...])
    up_pre = contract_last(x[:, :width], weights[1][...])
    for copy in second:
        copy.wait()
    back_proj = contract_last(q[...], weights[2][...])
    _, weight = slot_facts(x[:, width:])
    squash = jax.nn.sigmoid(sharpness * gate_pre)
    gated = gate_pre * squash
    more = up_pre + 1.0
    delta = weight * back_proj
    up_delta = (delta * gated).astype(jnp.bfloat16)
    slope = more * (squash + sharpness * gated * (1.0 - squash))
    gate_delta = (delta * slope).astype(jnp.bfloat16)
    act_scaled = (more * gated * weight).astype(jnp.bfloat16)
    for copy in third:
        copy.wait()
    for i, (left, right) in enumerate(
        ((gate_delta, x[:, :width]), (up_delta, x[:, :width]), (act_scaled, q[...]))
    ):
        total = contract_first(left, right)
        if with_start:
            total = total + held[i][...]
        outs[i][...] = total.astype(outs[i].dtype)


def combine_kernel(place_ref, facts_ref, *refs, routes, outer, inner):
    backs, (grad_ref, prob_ref) = refs[:-2], refs[-2:]
    rows = facts_ref.shape[0]
    capacity, wide = backs[0].shape
    width = wide - lanes
    facts = facts_ref[...].astype(jnp.float32)
    slot = iota((rows, capacity), 1).astype(jnp.float32)
    lane = iota((rows, lanes), 1)
    total = jnp.zeros((rows, width), jnp.float32)
    pairs = jnp.zeros((rows, lanes), jnp.float32)
    for p, back in enumerate(backs):
        expert = partner(place_ref[0], p % outer, p // outer, outer, inner)
        table = jnp.zeros((rows, capacity), jnp.float32)
        where_k = jnp.zeros((rows, 1), jnp.float32) - 1.0
        for k in range(routes):
            mine = facts[:, k : k + 1] == expert
            rank = jnp.where(mine, facts[:, routes + k : routes + k + 1], -1.0)
            table = table + (slot == rank).astype(jnp.float32)
            where_k = jnp.where(mine, float(k), where_k)
        table = table.astype(jnp.bfloat16)
        total = total + jnp.dot(table, back[:, :width], preferred_element_type=jnp.float32)
        term = lane_sum(
            jnp.dot(table, back[:, width:], preferred_element_type=jnp.float32), 0, 2
        )
        pairs = pairs + jnp.where(lane.astype(jnp.float32) == where_k, term, 0.0)
    grad_ref[...] = total.astype(jnp.bfloat16)
    prob_ref[...] = pairs.T[:routes]


def on_device(
    grad_out, tokens, probs, expert_ids, priority, cap_counts, gate_weight, up_weight, down_weight,
    *, outer,
):
    ep_size = lax.axis_size("ep")
    dp_size = lax.axis_size("dp")
    inner = ep_size // outer
    ep_rank = lax.axis_index("ep").astype(jnp.int32)
    rank = lax.axis_index("dp").reshape(1).astype(jnp.int32)
    tok_rows, model_width = tokens.shape
    routes = expert_ids.shape[1]
    hidden = gate_weight.shape[1]
    quarter = hidden // dp_size
    capacity = 5 * routes * tok_rows // (4 * ep_size)
    block = outer * capacity
    wide = model_width + lanes
    w_gate, w_up, w_down = gate_weight[0], up_weight[0], down_weight[0]
    bf16, f32 = jnp.bfloat16, jnp.float32
    shape = jax.ShapeDtypeStruct
    vmem = pl.BlockSpec(memory_space=pltpu.VMEM)
    smem = pl.BlockSpec(memory_space=pltpu.SMEM)
    hbm = pl.BlockSpec(memory_space=pltpu.HBM)

    token_x, token_q = pl.pallas_call(
        functools.partial(prep_kernel, experts=ep_size),
        out_shape=(shape((tok_rows, wide), bf16), shape((tok_rows, model_width), bf16)),
        in_specs=[smem] + [vmem] * 5,
        out_specs=(vmem,) * 2,
        compiler_params=params(),
        name="prep",
    )(cap_counts, expert_ids.T, priority, probs.T, grad_out, tokens)

    def move(rows, target):
        pairs = []
        for zz in range(outer):
            for i in range(inner):
                to = target(zz, i)
                if to is not None:
                    pairs.append((zz * inner + i, to[0] * inner + to[1]))
        return lax.ppermute(rows, "ep", pairs)

    def gather_near(rows):
        if outer != 4:
            return []
        below = move(rows, lambda zz, i: (zz + 1, i) if zz + 1 < outer else None)
        above = move(rows, lambda zz, i: (zz - 1, i) if zz else None)
        return [below, above]

    def gather_far(rows, near):
        if not near:
            back = lambda s: lambda zz, i: ((zz + s) % outer, i)
            return [rows] + [move(rows, back(s)) for s in range(1, outer)]
        below, above = near
        mixed = jnp.where(ep_rank < 2 * inner, below, above)
        across = move(mixed, lambda zz, i: {1: (3, i), 2: (0, i)}.get(zz))
        down = move(above, lambda zz, i: (zz - 1, i) if zz in (1, 2) else None)
        up = move(below, lambda zz, i: (zz + 1, i) if zz in (1, 2) else None)
        return [rows, below, above, down, up, across]

    spot = ep_rank.reshape(1)

    def x_slots(chunks):
        return pl.pallas_call(
            functools.partial(
                x_slots_kernel, outer=outer, inner=inner, capacity=capacity, routes=routes
            ),
            out_shape=(shape((block, wide), bf16),) * inner
            + (shape((outer * tok_rows, inner * block), bf16),),
            in_specs=[smem] + [vmem] * len(chunks),
            out_specs=(vmem,) * (inner + 1),
            compiler_params=params(),
            name="x_slots",
        )(spot, *chunks)

    def q_slots(table, chunks):
        return pl.pallas_call(
            functools.partial(q_slots_kernel, outer=outer, inner=inner),
            out_shape=(shape((block, model_width), bf16),) * inner,
            in_specs=[smem] + [vmem] * (1 + len(chunks)),
            out_specs=(vmem,) * inner,
            compiler_params=params(),
            name="q_slots",
        )(spot, table, *chunks)

    def exchange_inner(parts):
        step = lambda d: lambda zz, i: (zz, (i + d) % inner)
        got = [move(parts[d], step(d)) for d in range(1, inner)]
        return got[0] if inner == 2 else jnp.concatenate(got, axis=0)

    def swap(rows, step):
        return lax.ppermute(rows, "dp", [(d, d ^ step) for d in range(dp_size)])

    def x_part(rows, tiles):
        count = rows.shape[0]
        turn = lambda j, r: ((r[0] + j) % dp_size, 0)
        out = pl.BlockSpec((1, count, quarter), lambda j, r: (j, 0, 0))
        return pl.pallas_call(
            x_kernel,
            grid_spec=pltpu.PrefetchScalarGridSpec(
                num_scalar_prefetch=1,
                grid=(tiles,),
                in_specs=[
                    pl.BlockSpec((count, wide), lambda j, r: (0, 0)),
                    pl.BlockSpec((quarter, model_width), turn),
                    pl.BlockSpec((quarter, model_width), turn),
                ],
                out_specs=(out,) * 3,
            ),
            out_shape=(shape((tiles, count, quarter), bf16),) * 3,
            compiler_params=params(),
            cost_estimate=pl.CostEstimate(
                flops=4 * count * model_width * quarter * tiles,
                bytes_accessed=2 * count * wide + 4 * tiles * quarter * model_width,
                transcendentals=tiles * count * quarter,
            ),
            name="x_part",
        )(rank, rows, w_gate, w_up)

    def q_part(rows_q, rows_x, parts):
        count = rows_q.shape[0]
        turn = lambda j, r: ((r[0] + j) % dp_size, 0)
        tile = pl.BlockSpec((1, count, quarter), lambda j, r: (j, 0, 0))
        return pl.pallas_call(
            q_kernel,
            grid_spec=pltpu.PrefetchScalarGridSpec(
                num_scalar_prefetch=1,
                grid=(dp_size,),
                in_specs=[
                    pl.BlockSpec((count, model_width), lambda j, r: (0, 0)),
                    pl.BlockSpec((count, lanes), lambda j, r: (0, model_width // lanes)),
                    pl.BlockSpec((quarter, model_width), turn),
                    pl.BlockSpec((quarter, model_width), turn),
                    pl.BlockSpec((quarter, model_width), turn),
                    tile,
                    tile,
                    tile,
                ],
                out_specs=pl.BlockSpec((count, wide), lambda j, r: (0, 0)),
                scratch_shapes=[
                    pltpu.VMEM((count, model_width), f32),
                    pltpu.VMEM((count, 1), f32),
                ],
            ),
            out_shape=shape((count, wide), bf16),
            compiler_params=params(),
            cost_estimate=pl.CostEstimate(
                flops=6 * count * model_width * hidden,
                bytes_accessed=6 * hidden * model_width,
                transcendentals=0,
            ),
            name="q_part",
        )(rank, rows_q, rows_x, w_gate, w_up, w_down, *parts)

    def weight_grads(blocks_x, blocks_q, start, out_type):
        counts = [b.shape[0] for b in blocks_x]
        if len(set(counts)) > 1:
            blocks_x, blocks_q = ([jnp.concatenate(b, axis=0)] for b in (blocks_x, blocks_q))
        count, rows = len(blocks_x), sum(counts)
        operands = [*blocks_x, *blocks_q, w_gate, w_up, w_down, *(start or ())]
        scratch = [pltpu.VMEM((rows, wide), bf16), pltpu.VMEM((rows, model_width), bf16)]
        scratch += [pltpu.VMEM((quarter, model_width), bf16)] * 3
        if start:
            scratch += [pltpu.VMEM((quarter, model_width), f32)] * 3
        scratch += [pltpu.SemaphoreType.DMA((len(operands),))]
        return pl.pallas_call(
            functools.partial(
                weight_kernel, blocks=count, rows=rows // count, with_start=start is not None
            ),
            out_shape=(shape((quarter, model_width), out_type),) * 3,
            in_specs=[smem] + [hbm] * len(operands),
            out_specs=(vmem,) * 3,
            scratch_shapes=scratch,
            compiler_params=params(),
            cost_estimate=pl.CostEstimate(
                flops=12 * rows * model_width * quarter,
                bytes_accessed=4 * rows * wide,
                transcendentals=rows * quarter,
            ),
            name="weight_grads",
        )(rank, *operands)

    half = dp_size // 2

    def replicas(rows):
        near = [rows]
        far = [swap(rows, half)]
        step = half // 2
        while step:
            near += [swap(b, step) for b in near]
            far += [swap(b, step) for b in far]
            step //= 2
        return near, far

    near_chunks_x = gather_near(token_x)
    near_chunks_q = gather_near(token_q)
    chunks_x = gather_far(token_x, near_chunks_x)
    chunks_q = gather_far(token_q, near_chunks_q)
    *sends_x, table = x_slots(chunks_x)
    other_x = exchange_inner(sends_x)
    sends_q = q_slots(table, chunks_q)
    other_q = exchange_inner(sends_q)
    same_x, same_q = sends_x[0], sends_q[0]
    near_sx, far_sx = replicas(same_x)
    near_sq, far_sq = replicas(same_q)
    near_ox, far_ox = replicas(other_x)
    near_oq, far_oq = replicas(other_q)

    same_parts = x_part(same_x, dp_size)
    same_back = q_part(same_q, same_x, same_parts)
    other_parts = x_part(other_x, dp_size)
    other_back = q_part(other_q, other_x, other_parts)
    backs = []
    for d in range(inner):
        source = same_back if d == 0 else other_back[(d - 1) * block : d * block]
        for s in range(outer):
            rows = source[s * capacity : (s + 1) * capacity]
            if d or s:
                home = lambda zz, i: ((zz - s) % outer, (i - d) % inner)
                rows = move(rows, home)
            backs.append(rows)
    sums = weight_grads(near_sx + near_ox, near_sq + near_oq, None, f32)
    sums = weight_grads(far_sx, far_sq, sums, f32)
    shares = weight_grads(far_ox, far_oq, sums, bf16)
    input_grad, prob_grad = pl.pallas_call(
        functools.partial(combine_kernel, routes=routes, outer=outer, inner=inner),
        grid=(1,),
        out_shape=(shape((tok_rows, model_width), bf16), shape((routes, tok_rows), f32)),
        in_specs=[
            smem,
            pl.BlockSpec((tok_rows, lanes), lambda j: (0, model_width // lanes)),
        ]
        + [pl.BlockSpec((capacity, wide), lambda j: (0, 0))] * len(backs),
        out_specs=(
            pl.BlockSpec((tok_rows, model_width), lambda j: (0, 0)),
            pl.BlockSpec((routes, tok_rows), lambda j: (0, 0)),
        ),
        compiler_params=params(),
        name="combine",
    )(spot, token_x, *backs)
    return (input_grad, prob_grad.T, *(share[None] for share in shares))


def outer_size(mesh):
    heights = {getattr(d, "coords", (0, 0, 0))[2] for d in mesh.devices.flat}
    return len(heights) if mesh.shape["ep"] % len(heights) == 0 else 1


def solution(mesh):
    def whole(*arrays):
        return on_device(*arrays, outer=outer_size(mesh))

    return jax.shard_map(
        whole,
        mesh=mesh,
        in_specs=(
            P(("ep", "dp"), None),
            P(("ep", "dp"), None),
            P(("ep", "dp"), None),
            P(("ep", "dp"), None),
            P(("ep", "dp"), None),
            P(),
            P("ep", None, None),
            P("ep", None, None),
            P("ep", None, None),
        ),
        out_specs=(
            P(("ep", "dp"), None),
            P(("ep", "dp"), None),
            P("ep", "dp", None),
            P("ep", "dp", None),
            P("ep", "dp", None),
        ),
        check_vma=False,
    )
```

```python
import functools
import math

import jax
import jax.numpy as jnp
from jax import lax
from jax.experimental import pallas as pl
from jax.experimental.pallas import tpu as pltpu
from jax.sharding import PartitionSpec as P


sharpness = 1.702
lanes = 128

params = functools.partial(pltpu.CompilerParams, vmem_limit_bytes=56 * 1024 * 1024)


def contract_last(first_op, second_op):
    return lax.dot_general(
        first_op, second_op, (((1,), (1,)), ((), ())), preferred_element_type=jnp.float32
    )


def contract_first(first_op, second_op):
    return lax.dot_general(
        first_op, second_op, (((0,), (0,)), ((), ())), preferred_element_type=jnp.float32
    )


def high_low(values):
    high = values.astype(jnp.bfloat16)
    return high, (values - high.astype(jnp.float32)).astype(jnp.bfloat16)


def iota(shape, dim):
    return lax.broadcasted_iota(jnp.int32, shape, dim)


def lane_sum(values, first, stop):
    lane = iota(values.shape, 1)
    return jnp.sum(jnp.where((lane >= first) & (lane < stop), values, 0.0), axis=1, keepdims=True)


def columns_of(rows_ref, count):
    n = rows_ref.shape[1]
    return [
        jnp.broadcast_to(rows_ref[k : k + 1, :].astype(jnp.float32), (n, n)).T
        for k in range(count)
    ]


def prep_kernel(cap_ref, ids_ref, order_ref, probs_ref, grad_ref, tok_ref, x_ref, q_ref, *, experts):
    rows, width = tok_ref.shape
    routes = ids_ref.shape[0]
    lane = iota((rows, lanes), 1)
    lane_f = lane.astype(jnp.float32)
    order = jnp.broadcast_to(order_ref[...].astype(jnp.float32), (rows, rows))
    earlier = (order < order.T).astype(jnp.bfloat16)
    ids = columns_of(ids_ref, routes)
    chances = columns_of(probs_ref, routes)
    hits = [lane_f == i for i in ids]
    routed = sum(h.astype(jnp.float32) for h in hits)
    before = jnp.dot(earlier, routed.astype(jnp.bfloat16), preferred_element_type=jnp.float32)
    limit = jnp.zeros((rows, lanes), jnp.float32)
    for e in range(experts):
        limit = jnp.where(lane == e, cap_ref[e].astype(jnp.float32), limit)
    grad = grad_ref[...]
    scale = jnp.maximum(jnp.max(jnp.abs(grad), axis=1, keepdims=True), 1.0)
    q_ref[...] = (grad / scale).astype(jnp.bfloat16)
    facts = jnp.zeros((rows, lanes), jnp.float32)
    for k in range(routes):
        rank = jnp.sum(jnp.where(hits[k], before, 0.0), axis=1, keepdims=True)
        most = jnp.sum(jnp.where(hits[k], limit, 0.0), axis=1, keepdims=True)
        high, low = (p.astype(jnp.float32) for p in high_low(chances[k]))
        facts = jnp.where(lane == k, ids[k], facts)
        facts = jnp.where(lane == routes + k, jnp.where(rank < most, rank, -1.0), facts)
        facts = jnp.where(lane == 2 * routes + k, high, facts)
        facts = jnp.where(lane == 3 * routes + k, low, facts)
    high, low = (s.astype(jnp.float32) for s in high_low(scale))
    facts = jnp.where(lane == 4 * routes, high, facts)
    facts = jnp.where(lane == 4 * routes + 1, low, facts)
    x_ref[:, :width] = tok_ref[...]
    x_ref[:, width:] = facts.astype(jnp.bfloat16)


def chunks_of(place_ref, refs, outer, inner):
    if len(refs) == outer:
        return jnp.concatenate([r[...] for r in refs], axis=0)
    own, below, above, down, up, across = refs
    z = lax.div(place_ref[0], inner)
    back = jnp.where(z == 0, across[...], below[...])
    ahead = jnp.where(z == outer - 1, across[...], above[...])
    middle = jnp.where(z < outer // 2, down[...], up[...])
    return jnp.concatenate([own[...], back, middle, ahead], axis=0)


def partner(ep_rank, steps, places, outer, inner):
    z = lax.rem(lax.div(ep_rank, inner) + steps, outer)
    return (z * inner + lax.rem(lax.rem(ep_rank, inner) + places, inner)).astype(jnp.float32)


def x_slots_kernel(place_ref, *refs, outer, inner, capacity, routes):
    outs = refs[-inner - 1 :]
    rows = chunks_of(place_ref, refs[: -inner - 1], outer, inner)
    count, wide = rows.shape
    width = wide - lanes
    block = outer * capacity
    facts = rows[:, width:].astype(jnp.float32)
    chunk = (iota((count, 1), 0) // (count // outer)).astype(jnp.float32)
    slot = iota((count, inner * block), 1).astype(jnp.float32)
    table = jnp.zeros((count, inner * block), jnp.float32)
    chance = jnp.zeros((count, inner * block), jnp.float32)
    for k in range(routes):
        expert = facts[:, k : k + 1]
        rank = facts[:, routes + k : routes + k + 1]
        prob = facts[:, 2 * routes + k : 2 * routes + k + 1]
        prob = prob + facts[:, 3 * routes + k : 3 * routes + k + 1]
        column = jnp.full((count, 1), -1.0, jnp.float32)
        for d in range(inner):
            mine = (expert == partner(place_ref[0], 0, d, outer, inner)) & (rank >= 0.0)
            column = jnp.where(mine, d * block + chunk * capacity + rank, column)
        hit = (slot == column).astype(jnp.float32)
        table = table + hit
        chance = chance + hit * prob
    table = table.astype(jnp.bfloat16)
    outs[-1][...] = table
    chance_high, chance_low = high_low(chance)
    lane = iota((count, lanes), 1)
    scales = jnp.where(
        lane == 2,
        facts[:, 4 * routes : 4 * routes + 1],
        jnp.where(lane == 3, facts[:, 4 * routes + 1 : 4 * routes + 2], 0.0),
    ).astype(jnp.bfloat16)
    kept = (
        contract_first(chance_high, (lane == 0).astype(jnp.bfloat16))
        + contract_first(chance_low, (lane == 1).astype(jnp.bfloat16))
        + contract_first(table, scales)
    ).astype(jnp.bfloat16)
    for d in range(inner):
        part = slice(d * block, (d + 1) * block)
        outs[d][:, :width] = contract_first(table[:, part], rows[:, :width]).astype(jnp.bfloat16)
        outs[d][:, width:] = kept[part]


def q_slots_kernel(place_ref, table_ref, *refs, outer, inner):
    outs = refs[-inner:]
    rows = chunks_of(place_ref, refs[:-inner], outer, inner)
    block = table_ref.shape[1] // inner
    for d in range(inner):
        part = table_ref[:, d * block : (d + 1) * block]
        outs[d][...] = contract_first(part, rows).astype(jnp.bfloat16)


def slot_facts(values):
    values = values.astype(jnp.float32)
    scale = lane_sum(values, 2, 4)
    return scale, scale * lane_sum(values, 0, 2)


def expert_kernel(x_ref, q_ref, gate_ref, up_ref, down_ref, gate_delta_ref, up_delta_ref,
                  act_ref, *refs):
    outs, (sum_ref, prob_ref) = refs[:-2], refs[-2:]
    step = pl.program_id(0)
    width = q_ref.shape[1]
    x = x_ref[:, :width]
    scale, weight = slot_facts(x_ref[:, width:])
    gate_pre = contract_last(x, gate_ref[...])
    up_pre = contract_last(x, up_ref[...])
    back_proj = contract_last(q_ref[...], down_ref[...])
    squash = jax.nn.sigmoid(sharpness * gate_pre)
    gated = gate_pre * squash
    more = up_pre + 1.0
    activated = more * gated
    delta = weight * back_proj
    up_delta = (delta * gated).astype(jnp.bfloat16)
    slope = more * (squash + sharpness * gated * (1.0 - squash))
    gate_delta = (delta * slope).astype(jnp.bfloat16)
    gate_delta_ref[...] = gate_delta
    up_delta_ref[...] = up_delta
    act_ref[...] = (activated * weight).astype(jnp.bfloat16)
    share = jnp.dot(gate_delta, gate_ref[...], preferred_element_type=jnp.float32) + jnp.dot(
        up_delta, up_ref[...], preferred_element_type=jnp.float32
    )
    term = jnp.sum(activated * back_proj, axis=1, keepdims=True)

    @pl.when(step == 0)
    def _():
        sum_ref[...] = share
        prob_ref[...] = term

    @pl.when(step > 0)
    def _():
        sum_ref[...] += share
        prob_ref[...] += term

    @pl.when(step == pl.num_programs(0) - 1)
    def _():
        high, low = (h.astype(jnp.float32) for h in high_low(scale * prob_ref[...]))
        lane = iota((sum_ref.shape[0], lanes), 1)
        facts = jnp.where(lane == 0, high, jnp.where(lane == 1, low, 0.0))
        rows = outs[0].shape[0]
        for i, out in enumerate(outs):
            part = slice(i * rows, (i + 1) * rows)
            out[:, :width] = sum_ref[part, :].astype(jnp.bfloat16)
            out[:, width:] = facts[part].astype(jnp.bfloat16)


def weight_kernel(rank_ref, *refs, blocks, ready, rows, with_start):
    x_hbm, refs = refs[:blocks], refs[blocks:]
    q_hbm, refs = refs[:blocks], refs[blocks:]
    delta_hbm, refs = refs[: 3 * ready], refs[3 * ready :]
    weights_hbm, refs = refs[:3], refs[3:]
    starts, refs = (refs[:3], refs[3:]) if with_start else ((), refs)
    outs, refs = refs[:3], refs[3:]
    x, q, gate_up, down, refs = *refs[:4], refs[4:]
    parts, refs = refs[:3], refs[3:]
    held = refs[:3] if with_start else ()
    sems = refs[-1]
    copies = []

    def fetch(source, target):
        copy = pltpu.make_async_copy(source, target, sems.at[len(copies)])
        copy.start()
        copies.append(copy)
        return copy

    quarter = down.shape[0]
    mine = pl.ds(rank_ref[0] * quarter, quarter)
    known = ready * rows
    first = [fetch(weights_hbm[0].at[mine, :], gate_up.at[pl.ds(0, quarter)])]
    first += [fetch(weights_hbm[1].at[mine, :], gate_up.at[pl.ds(quarter, quarter)])]
    first += [fetch(x_hbm[b], x.at[pl.ds(b * rows, rows)]) for b in range(ready, blocks)]
    second = [fetch(weights_hbm[2].at[mine, :], down)]
    second += [fetch(q_hbm[b], q.at[pl.ds(b * rows, rows)]) for b in range(ready, blocks)]
    third = []
    for b in range(ready):
        part = pl.ds(b * rows, rows)
        third += [fetch(x_hbm[b], x.at[part]), fetch(q_hbm[b], q.at[part])]
        for i in range(3):
            third += [fetch(delta_hbm[3 * b + i].at[:, mine], parts[i].at[part, :])]
    third += [fetch(s, h) for s, h in zip(starts, held)]
    for copy in first:
        copy.wait()
    width = q.shape[1]
    pre = contract_last(x[known:, :width], gate_up[...])
    for copy in second:
        copy.wait()
    back_proj = contract_last(q[known:], down[...])
    _, weight = slot_facts(x[known:, width:])
    gate_pre, more = pre[:, :quarter], pre[:, quarter:] + 1.0
    squash = jax.nn.sigmoid(sharpness * gate_pre)
    gated = gate_pre * squash
    delta = weight * back_proj
    slope = more * (squash + sharpness * gated * (1.0 - squash))
    parts[0][known:, :] = (delta * slope).astype(jnp.bfloat16)
    parts[1][known:, :] = (delta * gated).astype(jnp.bfloat16)
    parts[2][known:, :] = (more * gated * weight).astype(jnp.bfloat16)
    for copy in third:
        copy.wait()
    for i, right in enumerate((x[:, :width], x[:, :width], q[...])):
        total = contract_first(parts[i][...], right)
        if with_start:
            total = total + held[i][...]
        outs[i][...] = total.astype(outs[i].dtype)


def combine_kernel(place_ref, facts_ref, *refs, routes, outer, inner):
    backs, (grad_ref, prob_ref) = refs[:-2], refs[-2:]
    rows = facts_ref.shape[0]
    capacity, wide = backs[0].shape
    width = wide - lanes
    facts = facts_ref[...].astype(jnp.float32)
    slot = iota((rows, capacity), 1).astype(jnp.float32)
    lane = iota((rows, lanes), 1)
    total = jnp.zeros((rows, width), jnp.float32)
    pairs = jnp.zeros((rows, lanes), jnp.float32)
    for p, back in enumerate(backs):
        expert = partner(place_ref[0], p % outer, p // outer, outer, inner)
        table = jnp.zeros((rows, capacity), jnp.float32)
        where_k = jnp.zeros((rows, 1), jnp.float32) - 1.0
        for k in range(routes):
            mine = facts[:, k : k + 1] == expert
            rank = jnp.where(mine, facts[:, routes + k : routes + k + 1], -1.0)
            table = table + (slot == rank).astype(jnp.float32)
            where_k = jnp.where(mine, float(k), where_k)
        table = table.astype(jnp.bfloat16)
        total = total + jnp.dot(table, back[:, :width], preferred_element_type=jnp.float32)
        term = lane_sum(
            jnp.dot(table, back[:, width:], preferred_element_type=jnp.float32), 0, 2
        )
        pairs = pairs + jnp.where(lane.astype(jnp.float32) == where_k, term, 0.0)
    grad_ref[...] = total.astype(jnp.bfloat16)
    prob_ref[...] = pairs.T[:routes]


def on_device(
    grad_out, tokens, probs, expert_ids, priority, cap_counts, gate_weight, up_weight, down_weight,
    *, outer,
):
    ep_size = lax.axis_size("ep")
    dp_size = lax.axis_size("dp")
    inner = ep_size // outer
    ep_rank = lax.axis_index("ep").astype(jnp.int32)
    rank = lax.axis_index("dp").reshape(1).astype(jnp.int32)
    tok_rows, model_width = tokens.shape
    routes = expert_ids.shape[1]
    hidden = gate_weight.shape[1]
    quarter = hidden // dp_size
    capacity = 5 * routes * tok_rows // (4 * ep_size)
    block = outer * capacity
    wide = model_width + lanes
    w_gate, w_up, w_down = gate_weight[0], up_weight[0], down_weight[0]
    bf16, f32 = jnp.bfloat16, jnp.float32
    shape = jax.ShapeDtypeStruct
    vmem = pl.BlockSpec(memory_space=pltpu.VMEM)
    smem = pl.BlockSpec(memory_space=pltpu.SMEM)
    hbm = pl.BlockSpec(memory_space=pltpu.HBM)

    token_x, token_q = pl.pallas_call(
        functools.partial(prep_kernel, experts=ep_size),
        out_shape=(shape((tok_rows, wide), bf16), shape((tok_rows, model_width), bf16)),
        in_specs=[smem] + [vmem] * 5,
        out_specs=(vmem,) * 2,
        compiler_params=params(),
        name="prep",
    )(cap_counts, expert_ids.T, priority, probs.T, grad_out, tokens)

    def move(rows, target):
        pairs = []
        for zz in range(outer):
            for i in range(inner):
                to = target(zz, i)
                if to is not None:
                    pairs.append((zz * inner + i, to[0] * inner + to[1]))
        return lax.ppermute(rows, "ep", pairs)

    def gather_near(rows):
        if outer != 4:
            return []
        below = move(rows, lambda zz, i: (zz + 1, i) if zz + 1 < outer else None)
        above = move(rows, lambda zz, i: (zz - 1, i) if zz else None)
        return [below, above]

    def gather_far(rows, near):
        if not near:
            back = lambda s: lambda zz, i: ((zz + s) % outer, i)
            return [rows] + [move(rows, back(s)) for s in range(1, outer)]
        below, above = near
        mixed = jnp.where(ep_rank < 2 * inner, below, above)
        across = move(mixed, lambda zz, i: {1: (3, i), 2: (0, i)}.get(zz))
        down = move(above, lambda zz, i: (zz - 1, i) if zz in (1, 2) else None)
        up = move(below, lambda zz, i: (zz + 1, i) if zz in (1, 2) else None)
        return [rows, below, above, down, up, across]

    spot = ep_rank.reshape(1)

    def x_slots(chunks):
        return pl.pallas_call(
            functools.partial(
                x_slots_kernel, outer=outer, inner=inner, capacity=capacity, routes=routes
            ),
            out_shape=(shape((block, wide), bf16),) * inner
            + (shape((outer * tok_rows, inner * block), bf16),),
            in_specs=[smem] + [vmem] * len(chunks),
            out_specs=(vmem,) * (inner + 1),
            compiler_params=params(),
            name="x_slots",
        )(spot, *chunks)

    def q_slots(table, chunks):
        return pl.pallas_call(
            functools.partial(q_slots_kernel, outer=outer, inner=inner),
            out_shape=(shape((block, model_width), bf16),) * inner,
            in_specs=[smem] + [vmem] * (1 + len(chunks)),
            out_specs=(vmem,) * inner,
            compiler_params=params(),
            name="q_slots",
        )(spot, table, *chunks)

    def exchange_inner(parts):
        step = lambda d: lambda zz, i: (zz, (i + d) % inner)
        got = [move(parts[d], step(d)) for d in range(1, inner)]
        return got[0] if inner == 2 else jnp.concatenate(got, axis=0)

    def swap(rows, step):
        return lax.ppermute(rows, "dp", [(d, d ^ step) for d in range(dp_size)])

    def expert_part(rows_x, rows_q):
        count = rows_q.shape[0]
        tiles = next(n for n in (3, 4, 2, 1) if hidden % (n * lanes) == 0)
        size = hidden // tiles
        weights = pl.BlockSpec((size, model_width), lambda j: (j, 0))
        units = pl.BlockSpec((count, size), lambda j: (0, j))
        pieces = count // capacity
        results = pl.pallas_call(
            expert_kernel,
            grid=(tiles,),
            in_specs=[
                pl.BlockSpec((count, wide), lambda j: (0, 0)),
                pl.BlockSpec((count, model_width), lambda j: (0, 0)),
                weights,
                weights,
                weights,
            ],
            out_specs=[units] * 3 + [pl.BlockSpec((capacity, wide), lambda j: (0, 0))] * pieces,
            scratch_shapes=[
                pltpu.VMEM((count, model_width), f32),
                pltpu.VMEM((count, 1), f32),
            ],
            out_shape=[shape((count, hidden), bf16)] * 3
            + [shape((capacity, wide), bf16)] * pieces,
            compiler_params=params(),
            cost_estimate=pl.CostEstimate(
                flops=10 * count * model_width * hidden,
                bytes_accessed=6 * hidden * model_width,
                transcendentals=count * hidden,
            ),
            name="expert_part",
        )(rows_x, rows_q, w_gate, w_up, w_down)
        return results[:3], results[3:]

    def weight_grads(blocks_x, blocks_q, deltas, start, out_type):
        counts = [b.shape[0] for b in blocks_x]
        if len(set(counts)) > 1:
            size = math.gcd(*counts)
            cut = lambda bs: [b[i : i + size] for b in bs for i in range(0, b.shape[0], size)]
            blocks_x, blocks_q = cut(blocks_x), cut(blocks_q)
            if deltas:
                columns = [cut(c) for c in zip(*deltas)]
                deltas = list(zip(*columns))
        count, rows, ready = len(blocks_x), sum(counts), len(deltas)
        operands = [*blocks_x, *blocks_q, *sum(map(list, deltas), [])]
        operands += [w_gate, w_up, w_down, *(start or ())]
        scratch = [pltpu.VMEM((rows, wide), bf16), pltpu.VMEM((rows, model_width), bf16)]
        scratch += [pltpu.VMEM((2 * quarter, model_width), bf16)]
        scratch += [pltpu.VMEM((quarter, model_width), bf16)]
        scratch += [pltpu.VMEM((rows, quarter), bf16)] * 3
        if start:
            scratch += [pltpu.VMEM((quarter, model_width), f32)] * 3
        scratch += [pltpu.SemaphoreType.DMA((len(operands),))]
        return pl.pallas_call(
            functools.partial(
                weight_kernel,
                blocks=count,
                ready=ready,
                rows=rows // count,
                with_start=start is not None,
            ),
            out_shape=(shape((quarter, model_width), out_type),) * 3,
            in_specs=[smem] + [hbm] * len(operands),
            out_specs=(vmem,) * 3,
            scratch_shapes=scratch,
            compiler_params=params(),
            cost_estimate=pl.CostEstimate(
                flops=12 * rows * model_width * quarter,
                bytes_accessed=4 * rows * wide,
                transcendentals=rows * quarter,
            ),
            name="weight_grads",
        )(rank, *operands)

    half = dp_size // 2

    def replicas(rows):
        near = [rows]
        far = [swap(rows, half)]
        step = half // 2
        while step:
            near += [swap(b, step) for b in near]
            far += [swap(b, step) for b in far]
            step //= 2
        return near, far

    near_chunks_x = gather_near(token_x)
    near_chunks_q = gather_near(token_q)
    chunks_x = gather_far(token_x, near_chunks_x)
    chunks_q = gather_far(token_q, near_chunks_q)
    *sends_x, table = x_slots(chunks_x)
    other_x = exchange_inner(sends_x)
    sends_q = q_slots(table, chunks_q)
    other_q = exchange_inner(sends_q)
    same_x, same_q = sends_x[0], sends_q[0]
    near_sx, far_sx = replicas(same_x)
    near_sq, far_sq = replicas(same_q)
    near_ox, far_ox = replicas(other_x)
    near_oq, far_oq = replicas(other_q)

    same_deltas, same_back = expert_part(same_x, same_q)
    other_deltas, other_back = expert_part(other_x, other_q)
    backs = []
    for i, rows in enumerate([*same_back, *other_back]):
        d, s = i // outer, i % outer
        if i:
            home = lambda zz, ii: ((zz - s) % outer, (ii - d) % inner)
            rows = move(rows, home)
        backs.append(rows)
    sums = weight_grads(
        [near_sx[0], near_ox[0], *near_sx[1:], *near_ox[1:]],
        [near_sq[0], near_oq[0], *near_sq[1:], *near_oq[1:]],
        [same_deltas, other_deltas],
        None,
        f32,
    )
    sums = weight_grads(far_sx, far_sq, [], sums, f32)
    shares = weight_grads(far_ox, far_oq, [], sums, bf16)
    input_grad, prob_grad = pl.pallas_call(
        functools.partial(combine_kernel, routes=routes, outer=outer, inner=inner),
        grid=(1,),
        out_shape=(shape((tok_rows, model_width), bf16), shape((routes, tok_rows), f32)),
        in_specs=[
            smem,
            pl.BlockSpec((tok_rows, lanes), lambda j: (0, model_width // lanes)),
        ]
        + [pl.BlockSpec((capacity, wide), lambda j: (0, 0))] * len(backs),
        out_specs=(
            pl.BlockSpec((tok_rows, model_width), lambda j: (0, 0)),
            pl.BlockSpec((routes, tok_rows), lambda j: (0, 0)),
        ),
        compiler_params=params(),
        name="combine",
    )(spot, token_x, *backs)
    return (input_grad, prob_grad.T, *(share[None] for share in shares))


def outer_size(mesh):
    heights = {getattr(d, "coords", (0, 0, 0))[2] for d in mesh.devices.flat}
    return len(heights) if mesh.shape["ep"] % len(heights) == 0 else 1


def solution(mesh):
    def whole(*arrays):
        return on_device(*arrays, outer=outer_size(mesh))

    return jax.shard_map(
        whole,
        mesh=mesh,
        in_specs=(
            P(("ep", "dp"), None),
            P(("ep", "dp"), None),
            P(("ep", "dp"), None),
            P(("ep", "dp"), None),
            P(("ep", "dp"), None),
            P(),
            P("ep", None, None),
            P("ep", None, None),
            P("ep", None, None),
        ),
        out_specs=(
            P(("ep", "dp"), None),
            P(("ep", "dp"), None),
            P("ep", "dp", None),
            P("ep", "dp", None),
            P("ep", "dp", None),
        ),
        check_vma=False,
    )
```

```python
import functools
import math

import jax
import jax.numpy as jnp
from jax import lax
from jax.experimental import pallas as pl
from jax.experimental.pallas import tpu as pltpu
from jax.sharding import PartitionSpec as P


sharpness = 1.702
lanes = 128


def contract_last(first_op, second_op):
    return lax.dot_general(
        first_op, second_op, (((1,), (1,)), ((), ())), preferred_element_type=jnp.float32
    )


def contract_first(first_op, second_op):
    return lax.dot_general(
        first_op, second_op, (((0,), (0,)), ((), ())), preferred_element_type=jnp.float32
    )


def high_low(values):
    high = values.astype(jnp.bfloat16)
    return high, (values - high.astype(jnp.float32)).astype(jnp.bfloat16)


def iota(shape, dim):
    return lax.broadcasted_iota(jnp.int32, shape, dim)


def lane_sum(values, first, stop):
    lane = iota(values.shape, 1)
    return jnp.sum(jnp.where((lane >= first) & (lane < stop), values, 0.0), axis=1, keepdims=True)


def columns_of(rows_ref, count):
    n = rows_ref.shape[1]
    return [
        jnp.broadcast_to(rows_ref[k : k + 1, :].astype(jnp.float32), (n, n)).T
        for k in range(count)
    ]


def prep_kernel(cap_ref, ids_ref, order_ref, probs_ref, grad_ref, tok_ref, x_ref, q_ref, facts_ref,
                *, experts):
    rows, width = tok_ref.shape
    routes = ids_ref.shape[0]
    lane = iota((rows, lanes), 1)
    lane_f = lane.astype(jnp.float32)
    order = jnp.broadcast_to(order_ref[...].astype(jnp.float32), (rows, rows))
    earlier = (order < order.T).astype(jnp.bfloat16)
    ids = columns_of(ids_ref, routes)
    chances = columns_of(probs_ref, routes)
    hits = [lane_f == i for i in ids]
    routed = sum(h.astype(jnp.float32) for h in hits)
    before = jnp.dot(earlier, routed.astype(jnp.bfloat16), preferred_element_type=jnp.float32)
    limit = jnp.zeros((rows, lanes), jnp.float32)
    for e in range(experts):
        limit = jnp.where(lane == e, cap_ref[e].astype(jnp.float32), limit)
    grad = grad_ref[...]
    scale = jnp.maximum(jnp.max(jnp.abs(grad), axis=1, keepdims=True), 1.0)
    q_ref[...] = (grad / scale).astype(jnp.bfloat16)
    facts = jnp.zeros((rows, lanes), jnp.float32)
    for k in range(routes):
        rank = jnp.sum(jnp.where(hits[k], before, 0.0), axis=1, keepdims=True)
        most = jnp.sum(jnp.where(hits[k], limit, 0.0), axis=1, keepdims=True)
        high, low = (p.astype(jnp.float32) for p in high_low(chances[k]))
        facts = jnp.where(lane == k, ids[k], facts)
        facts = jnp.where(lane == routes + k, jnp.where(rank < most, rank, -1.0), facts)
        facts = jnp.where(lane == 2 * routes + k, high, facts)
        facts = jnp.where(lane == 3 * routes + k, low, facts)
    high, low = (s.astype(jnp.float32) for s in high_low(scale))
    facts = jnp.where(lane == 4 * routes, high, facts)
    facts = jnp.where(lane == 4 * routes + 1, low, facts)
    x_ref[:, :width] = tok_ref[...]
    facts = facts.astype(jnp.bfloat16)
    x_ref[:, width:] = facts
    facts_ref[...] = facts


def chunks_of(place_ref, refs, outer, inner):
    if len(refs) == outer:
        return jnp.concatenate([r[...] for r in refs], axis=0)
    own, below, above, down, up, across = refs
    z = lax.div(place_ref[0], inner)
    back = jnp.where(z == 0, across[...], below[...])
    ahead = jnp.where(z == outer - 1, across[...], above[...])
    middle = jnp.where(z < outer // 2, down[...], up[...])
    return jnp.concatenate([own[...], back, middle, ahead], axis=0)


def partner(ep_rank, steps, places, outer, inner):
    z = lax.rem(lax.div(ep_rank, inner) + steps, outer)
    return (z * inner + lax.rem(lax.rem(ep_rank, inner) + places, inner)).astype(jnp.float32)


def x_slots_kernel(place_ref, *refs, outer, inner, capacity, routes):
    outs = refs[-inner - 1 :]
    rows = chunks_of(place_ref, refs[: -inner - 1], outer, inner)
    count, wide = rows.shape
    width = wide - lanes
    block = outer * capacity
    facts = rows[:, width:].astype(jnp.float32)
    chunk = (iota((count, 1), 0) // (count // outer)).astype(jnp.float32)
    slot = iota((count, inner * block), 1).astype(jnp.float32)
    table = jnp.zeros((count, inner * block), jnp.float32)
    chances = [jnp.zeros((count, 1), jnp.float32)] * inner
    for k in range(routes):
        expert = facts[:, k : k + 1]
        rank = facts[:, routes + k : routes + k + 1]
        prob = facts[:, 2 * routes + k : 2 * routes + k + 1]
        prob = prob + facts[:, 3 * routes + k : 3 * routes + k + 1]
        column = jnp.full((count, 1), -1.0, jnp.float32)
        for d in range(inner):
            mine = (expert == partner(place_ref[0], 0, d, outer, inner)) & (rank >= 0.0)
            column = jnp.where(mine, d * block + chunk * capacity + rank, column)
            chances[d] = jnp.where(mine, prob, chances[d])
        table = table + (slot == column).astype(jnp.float32)
    table = table.astype(jnp.bfloat16)
    outs[-1][...] = table
    lane = iota((count, lanes), 1)
    scales = jnp.where(
        lane == 2,
        facts[:, 4 * routes : 4 * routes + 1],
        jnp.where(lane == 3, facts[:, 4 * routes + 1 : 4 * routes + 2], 0.0),
    )
    for d in range(inner):
        part = table[:, d * block : (d + 1) * block]
        high, low = (h.astype(jnp.float32) for h in high_low(chances[d]))
        kept = jnp.where(lane == 0, high, jnp.where(lane == 1, low, scales)).astype(jnp.bfloat16)
        outs[d][:, :width] = contract_first(part, rows[:, :width]).astype(jnp.bfloat16)
        outs[d][:, width:] = contract_first(part, kept).astype(jnp.bfloat16)


def q_slots_kernel(place_ref, table_ref, *refs, outer, inner):
    outs = refs[-inner:]
    rows = chunks_of(place_ref, refs[:-inner], outer, inner)
    block = table_ref.shape[1] // inner
    for d in range(inner):
        part = table_ref[:, d * block : (d + 1) * block]
        outs[d][...] = contract_first(part, rows).astype(jnp.bfloat16)


def slot_facts(values):
    values = values.astype(jnp.float32)
    scale = lane_sum(values, 2, 4)
    return scale, scale * lane_sum(values, 0, 2)


class Copies:
    def __init__(self, sems):
        self.sems, self.count = sems, 0

    def start(self, source, target):
        copy = pltpu.make_async_copy(source, target, self.sems.at[self.count])
        copy.start()
        self.count += 1
        return copy


def wait_all(copies):
    for copy in copies:
        copy.wait()


def expert_kernel(rank_ref, x_hbm, q_hbm, *refs, tiles):
    weights_hbm, refs = refs[:3], refs[3:]
    owns_hbm, refs = refs[:3], refs[3:]
    *refs, x, q, gate, up, down, every_gate, every_up, every_act, sum_ref, prob_ref, sems, own_sems = refs
    outs_hbm, outs = refs[: len(refs) // 2], refs[len(refs) // 2 :]
    weights, alls = (gate, up, down), (every_gate, every_up, every_act)
    size, width = gate.shape[1:]
    copies = Copies(own_sems)

    def tile_copy(i, tile):
        part = pl.ds(tile * size, size)
        return pltpu.make_async_copy(
            weights_hbm[i].at[part, :], weights[i].at[tile], sems.at[i, tile]
        )

    loads = [copies.start(x_hbm, x)]
    tile_copy(0, 0).start()
    tile_copy(1, 0).start()
    loads.append(copies.start(q_hbm, q))
    tile_copy(2, 0).start()
    for tile in range(1, tiles):
        for i in range(3):
            tile_copy(i, tile).start()
    loads[0].wait()
    scale, weight = slot_facts(x[:, width:])
    sum_ref[...] = jnp.zeros_like(sum_ref)
    prob_ref[...] = jnp.zeros_like(prob_ref)
    loads[1].wait()

    def step(tile, carry):
        units = pl.ds(pl.multiple_of(tile * size, lanes), size)
        rows = x[:, :width]
        tile_copy(0, tile).wait()
        gate_pre = contract_last(rows, gate[tile])
        tile_copy(1, tile).wait()
        up_pre = contract_last(rows, up[tile])
        tile_copy(2, tile).wait()
        back_proj = contract_last(q[...], down[tile])
        squash = jax.nn.sigmoid(sharpness * gate_pre)
        gated = gate_pre * squash
        more = up_pre + 1.0
        activated = more * gated
        delta = weight * back_proj
        up_delta = (delta * gated).astype(jnp.bfloat16)
        slope = more * (squash + sharpness * gated * (1.0 - squash))
        gate_delta = (delta * slope).astype(jnp.bfloat16)
        every_gate[:, units] = gate_delta
        every_up[:, units] = up_delta
        every_act[:, units] = (activated * weight).astype(jnp.bfloat16)
        share = jnp.dot(gate_delta, gate[tile], preferred_element_type=jnp.float32)
        share = share + jnp.dot(up_delta, up[tile], preferred_element_type=jnp.float32)
        sum_ref[...] += share
        prob_ref[...] += jnp.sum(activated * back_proj, axis=1, keepdims=True)
        return carry

    lax.fori_loop(0, tiles, step, 0)
    high, low = (h.astype(jnp.float32) for h in high_low(scale * prob_ref[...]))
    lane = iota((sum_ref.shape[0], lanes), 1)
    facts = jnp.where(lane == 0, high, jnp.where(lane == 1, low, 0.0))
    stores = []
    for i, (out, out_hbm) in enumerate(zip(outs, outs_hbm)):
        rows = out.shape[0]
        part = slice(i * rows, (i + 1) * rows)
        out[:, :width] = sum_ref[part, :].astype(jnp.bfloat16)
        out[:, width:] = facts[part].astype(jnp.bfloat16)
        stores.append(copies.start(out, out_hbm))
    quarter = owns_hbm[0].shape[1]
    mine = pl.ds(pl.multiple_of(rank_ref[0] * quarter, lanes), quarter)
    stores += [copies.start(every.at[:, mine], own) for every, own in zip(alls, owns_hbm)]
    wait_all(stores)


def weight_kernel(rank_ref, *refs, blocks, ready, rows, with_start):
    x_hbm, refs = refs[:blocks], refs[blocks:]
    q_hbm, refs = refs[:blocks], refs[blocks:]
    deltas_hbm, refs = refs[: 3 * ready], refs[3 * ready :]
    weights_hbm, refs = refs[:3], refs[3:]
    starts_hbm, refs = (refs[:3], refs[3:]) if with_start else ((), refs)
    outs_hbm, refs = refs[:3], refs[3:]
    x, q, gate_up, down, refs = *refs[:4], refs[4:]
    parts, sums, sems = refs[:3], refs[3:6], refs[6]
    copies = Copies(sems)
    quarter = down.shape[0]
    mine = pl.ds(rank_ref[0] * quarter, quarter)
    known = ready * rows
    place = lambda b: pl.ds(b * rows, rows)
    first = [copies.start(x_hbm[b], x.at[place(b)]) for b in range(ready, blocks)]
    for i in range(2):
        target = gate_up.at[pl.ds(i * quarter, quarter)]
        first.append(copies.start(weights_hbm[i].at[mine, :], target))
    second = [copies.start(q_hbm[b], q.at[place(b)]) for b in range(ready, blocks)]
    second.append(copies.start(weights_hbm[2].at[mine, :], down))
    third = []
    for b in range(ready):
        third += [copies.start(x_hbm[b], x.at[place(b)]), copies.start(q_hbm[b], q.at[place(b)])]
        third += [
            copies.start(deltas_hbm[3 * b + i], parts[i].at[place(b)]) for i in range(3)
        ]
    third += [copies.start(s, h) for s, h in zip(starts_hbm, sums)]
    wait_all(first)
    width = q.shape[1]
    pre = contract_last(x[known:, :width], gate_up[...])
    wait_all(second)
    back_proj = contract_last(q[known:], down[...])
    _, weight = slot_facts(x[known:, width:])
    gate_pre, more = pre[:, :quarter], pre[:, quarter:] + 1.0
    squash = jax.nn.sigmoid(sharpness * gate_pre)
    gated = gate_pre * squash
    delta = weight * back_proj
    slope = more * (squash + sharpness * gated * (1.0 - squash))
    parts[0][known:, :] = (delta * slope).astype(jnp.bfloat16)
    parts[1][known:, :] = (delta * gated).astype(jnp.bfloat16)
    parts[2][known:, :] = (more * gated * weight).astype(jnp.bfloat16)
    wait_all(third)
    stores = []
    for i, right in enumerate((x[:, :width], x[:, :width], q[...])):
        total = contract_first(parts[i][...], right)
        if with_start:
            total = total + sums[i][...].astype(jnp.float32)
        sums[i][...] = total.astype(jnp.bfloat16)
        stores.append(copies.start(sums[i], outs_hbm[i]))
    wait_all(stores)


def combine_kernel(place_ref, facts_ref, *refs, routes, outer, inner):
    backs, (grad_ref, prob_ref) = refs[:-2], refs[-2:]
    rows = facts_ref.shape[0]
    capacity, wide = backs[0].shape
    width = wide - lanes
    facts = facts_ref[...].astype(jnp.float32)
    slot = iota((rows, capacity), 1).astype(jnp.float32)
    lane = iota((rows, lanes), 1)
    total = jnp.zeros((rows, width), jnp.float32)
    pairs = jnp.zeros((rows, lanes), jnp.float32)
    for p, back in enumerate(backs):
        expert = partner(place_ref[0], p % outer, p // outer, outer, inner)
        table = jnp.zeros((rows, capacity), jnp.float32)
        where_k = jnp.zeros((rows, 1), jnp.float32) - 1.0
        for k in range(routes):
            mine = facts[:, k : k + 1] == expert
            rank = jnp.where(mine, facts[:, routes + k : routes + k + 1], -1.0)
            table = table + (slot == rank).astype(jnp.float32)
            where_k = jnp.where(mine, float(k), where_k)
        table = table.astype(jnp.bfloat16)
        total = total + jnp.dot(table, back[:, :width], preferred_element_type=jnp.float32)
        term = lane_sum(
            jnp.dot(table, back[:, width:], preferred_element_type=jnp.float32), 0, 2
        )
        pairs = pairs + jnp.where(lane.astype(jnp.float32) == where_k, term, 0.0)
    grad_ref[...] = total.astype(jnp.bfloat16)
    prob_ref[...] = pairs.T[:routes]


def on_device(
    grad_out, tokens, probs, expert_ids, priority, cap_counts, gate_weight, up_weight, down_weight,
    *, outer,
):
    ep_size = lax.axis_size("ep")
    dp_size = lax.axis_size("dp")
    inner = ep_size // outer
    ep_rank = lax.axis_index("ep").astype(jnp.int32)
    rank = lax.axis_index("dp").reshape(1).astype(jnp.int32)
    tok_rows, model_width = tokens.shape
    routes = expert_ids.shape[1]
    hidden = gate_weight.shape[1]
    quarter = hidden // dp_size
    capacity = 5 * routes * tok_rows // (4 * ep_size)
    block = outer * capacity
    wide = model_width + lanes
    w_gate, w_up, w_down = gate_weight[0], up_weight[0], down_weight[0]
    bf16, f32 = jnp.bfloat16, jnp.float32
    shape = jax.ShapeDtypeStruct
    vmem = pl.BlockSpec(memory_space=pltpu.VMEM)
    smem = pl.BlockSpec(memory_space=pltpu.SMEM)
    hbm = pl.BlockSpec(memory_space=pltpu.HBM)

    token_x, token_q, token_facts = pl.pallas_call(
        functools.partial(prep_kernel, experts=ep_size),
        out_shape=(
            shape((tok_rows, wide), bf16),
            shape((tok_rows, model_width), bf16),
            shape((tok_rows, lanes), bf16),
        ),
        in_specs=[smem] + [vmem] * 5,
        out_specs=(vmem,) * 3,
        compiler_params=pltpu.CompilerParams(vmem_limit_bytes=24 << 20),
        name="prep",
    )(cap_counts, expert_ids.T, priority, probs.T, grad_out, tokens)

    def move(rows, target):
        pairs = []
        for zz in range(outer):
            for i in range(inner):
                to = target(zz, i)
                if to is not None:
                    pairs.append((zz * inner + i, to[0] * inner + to[1]))
        return lax.ppermute(rows, "ep", pairs)

    def gather_near(rows):
        if outer != 4:
            return []
        below = move(rows, lambda zz, i: (zz + 1, i) if zz + 1 < outer else None)
        above = move(rows, lambda zz, i: (zz - 1, i) if zz else None)
        return [below, above]

    def gather_far(rows, near):
        if not near:
            back = lambda s: lambda zz, i: ((zz + s) % outer, i)
            return [rows] + [move(rows, back(s)) for s in range(1, outer)]
        below, above = near
        mixed = jnp.where(ep_rank < 2 * inner, below, above)
        across = move(mixed, lambda zz, i: {1: (3, i), 2: (0, i)}.get(zz))
        down = move(above, lambda zz, i: (zz - 1, i) if zz in (1, 2) else None)
        up = move(below, lambda zz, i: (zz + 1, i) if zz in (1, 2) else None)
        return [rows, below, above, down, up, across]

    spot = ep_rank.reshape(1)

    def x_slots(chunks):
        return pl.pallas_call(
            functools.partial(
                x_slots_kernel, outer=outer, inner=inner, capacity=capacity, routes=routes
            ),
            out_shape=(shape((block, wide), bf16),) * inner
            + (shape((outer * tok_rows, inner * block), bf16),),
            in_specs=[smem] + [vmem] * len(chunks),
            out_specs=(vmem,) * (inner + 1),
            compiler_params=pltpu.CompilerParams(vmem_limit_bytes=24 << 20),
            name="x_slots",
        )(spot, *chunks)

    def q_slots(table, chunks):
        return pl.pallas_call(
            functools.partial(q_slots_kernel, outer=outer, inner=inner),
            out_shape=(shape((block, model_width), bf16),) * inner,
            in_specs=[smem] + [vmem] * (1 + len(chunks)),
            out_specs=(vmem,) * inner,
            compiler_params=pltpu.CompilerParams(vmem_limit_bytes=24 << 20),
            name="q_slots",
        )(spot, table, *chunks)

    def exchange_inner(parts):
        step = lambda d: lambda zz, i: (zz, (i + d) % inner)
        got = [move(parts[d], step(d)) for d in range(1, inner)]
        return got[0] if inner == 2 else jnp.concatenate(got, axis=0)

    def swap(rows, step):
        return lax.ppermute(rows, "dp", [(d, d ^ step) for d in range(dp_size)])

    def expert_part(rows_x, rows_q):
        count = rows_q.shape[0]
        tiles = next(n for n in (3, 4, 2, 1) if hidden % (n * lanes) == 0)
        pieces = count // capacity
        size = hidden // tiles
        results = pl.pallas_call(
            functools.partial(expert_kernel, tiles=tiles),
            in_specs=[smem] + [hbm] * 5,
            out_specs=[hbm] * (3 + pieces),
            scratch_shapes=[pltpu.VMEM((capacity, wide), bf16)] * pieces
            + [pltpu.VMEM((count, wide), bf16), pltpu.VMEM((count, model_width), bf16)]
            + [pltpu.VMEM((tiles, size, model_width), bf16)] * 3
            + [pltpu.VMEM((count, hidden), bf16)] * 3
            + [pltpu.VMEM((count, model_width), f32), pltpu.VMEM((count, 1), f32)]
            + [pltpu.SemaphoreType.DMA((3, tiles)), pltpu.SemaphoreType.DMA((pieces + 5,))],
            out_shape=[shape((count, quarter), bf16)] * 3
            + [shape((capacity, wide), bf16)] * pieces,
            compiler_params=pltpu.CompilerParams(vmem_limit_bytes=48 << 20),
            cost_estimate=pl.CostEstimate(
                flops=10 * count * model_width * hidden,
                bytes_accessed=6 * hidden * model_width,
                transcendentals=count * hidden,
            ),
            name="expert_part",
        )(rank, rows_x, rows_q, w_gate, w_up, w_down)
        return results[:3], results[3:]

    def weight_grads(blocks_x, blocks_q, deltas, start):
        counts = [b.shape[0] for b in blocks_x]
        if len(set(counts)) > 1:
            size = math.gcd(*counts)
            cut = lambda bs: [b[i : i + size] for b in bs for i in range(0, b.shape[0], size)]
            blocks_x, blocks_q = cut(blocks_x), cut(blocks_q)
            if deltas:
                columns = [cut(c) for c in zip(*deltas)]
                deltas = list(zip(*columns))
        count, rows, ready = len(blocks_x), sum(counts), len(deltas)
        operands = [*blocks_x, *blocks_q, *sum(map(list, deltas), [])]
        operands += [w_gate, w_up, w_down, *(start or ())]
        scratch = [pltpu.VMEM((rows, wide), bf16), pltpu.VMEM((rows, model_width), bf16)]
        scratch += [pltpu.VMEM((2 * quarter, model_width), bf16)]
        scratch += [pltpu.VMEM((quarter, model_width), bf16)]
        scratch += [pltpu.VMEM((rows, quarter), bf16)] * 3
        scratch += [pltpu.VMEM((quarter, model_width), bf16)] * 3
        scratch += [pltpu.SemaphoreType.DMA((len(operands) + 3,))]
        return pl.pallas_call(
            functools.partial(
                weight_kernel,
                blocks=count,
                ready=ready,
                rows=rows // count,
                with_start=start is not None,
            ),
            out_shape=(shape((quarter, model_width), bf16),) * 3,
            in_specs=[smem] + [hbm] * len(operands),
            out_specs=(hbm,) * 3,
            scratch_shapes=scratch,
            compiler_params=pltpu.CompilerParams(vmem_limit_bytes=48 << 20),
            cost_estimate=pl.CostEstimate(
                flops=12 * rows * model_width * quarter,
                bytes_accessed=4 * rows * wide,
                transcendentals=rows * quarter,
            ),
            name="weight_grads",
        )(rank, *operands)

    half = dp_size // 2

    def replicas(rows):
        near = [rows]
        far = [swap(rows, half)]
        step = half // 2
        while step:
            near += [swap(b, step) for b in near]
            far += [swap(b, step) for b in far]
            step //= 2
        return near, far

    near_chunks_x = gather_near(token_x)
    near_chunks_q = gather_near(token_q)
    chunks_x = gather_far(token_x, near_chunks_x)
    chunks_q = gather_far(token_q, near_chunks_q)
    *sends_x, table = x_slots(chunks_x)
    other_x = exchange_inner(sends_x)
    sends_q = q_slots(table, chunks_q)
    other_q = exchange_inner(sends_q)
    same_x, same_q = sends_x[0], sends_q[0]
    near_sx, far_sx = replicas(same_x)
    near_sq, far_sq = replicas(same_q)
    near_ox, far_ox = replicas(other_x)
    near_oq, far_oq = replicas(other_q)

    same_deltas, same_back = expert_part(same_x, same_q)
    other_deltas, other_back = expert_part(other_x, other_q)
    backs = []
    for i, rows in enumerate([*same_back, *other_back]):
        d, s = i // outer, i % outer
        if i:
            home = lambda zz, ii: ((zz - s) % outer, (ii - d) % inner)
            rows = move(rows, home)
        backs.append(rows)
    sums = weight_grads(near_sx, near_sq, [same_deltas], None)
    sums = weight_grads(near_ox, near_oq, [other_deltas], sums)
    sums = weight_grads(far_sx, far_sq, [], sums)
    shares = weight_grads(far_ox, far_oq, [], sums)
    input_grad, prob_grad = pl.pallas_call(
        functools.partial(combine_kernel, routes=routes, outer=outer, inner=inner),
        out_shape=(shape((tok_rows, model_width), bf16), shape((routes, tok_rows), f32)),
        in_specs=[smem] + [vmem] * (1 + len(backs)),
        out_specs=(vmem,) * 2,
        compiler_params=pltpu.CompilerParams(vmem_limit_bytes=24 << 20),
        name="combine",
    )(spot, token_facts, *backs)
    return (input_grad, prob_grad.T, *(share[None] for share in shares))


def outer_size(mesh):
    heights = {getattr(d, "coords", (0, 0, 0))[2] for d in mesh.devices.flat}
    return len(heights) if mesh.shape["ep"] % len(heights) == 0 else 1


def solution(mesh):
    def whole(*arrays):
        return on_device(*arrays, outer=outer_size(mesh))

    return jax.shard_map(
        whole,
        mesh=mesh,
        in_specs=(
            P(("ep", "dp"), None),
            P(("ep", "dp"), None),
            P(("ep", "dp"), None),
            P(("ep", "dp"), None),
            P(("ep", "dp"), None),
            P(),
            P("ep", None, None),
            P("ep", None, None),
            P("ep", None, None),
        ),
        out_specs=(
            P(("ep", "dp"), None),
            P(("ep", "dp"), None),
            P("ep", "dp", None),
            P("ep", "dp", None),
            P("ep", "dp", None),
        ),
        check_vma=False,
    )
```

```python
import functools
import math

import jax
import jax.numpy as jnp
from jax import lax
from jax.experimental import pallas as pl
from jax.experimental.pallas import tpu as pltpu
from jax.sharding import PartitionSpec as P


sharpness = 1.702
lanes = 128


def contract_last(first_op, second_op):
    return lax.dot_general(
        first_op, second_op, (((1,), (1,)), ((), ())), preferred_element_type=jnp.float32
    )


def contract_first(first_op, second_op):
    return lax.dot_general(
        first_op, second_op, (((0,), (0,)), ((), ())), preferred_element_type=jnp.float32
    )


def in_hbm(*arrays):
    return [pltpu.with_memory_space_constraint(a, pltpu.HBM) for a in arrays]


def high_low(values):
    high = values.astype(jnp.bfloat16)
    return high, (values - high.astype(jnp.float32)).astype(jnp.bfloat16)


def iota(shape, dim):
    return lax.broadcasted_iota(jnp.int32, shape, dim)


def lane_sum(values, first, stop):
    lane = iota(values.shape, 1)
    return jnp.sum(jnp.where((lane >= first) & (lane < stop), values, 0.0), axis=1, keepdims=True)


def columns_of(rows_ref, count):
    n = rows_ref.shape[1]
    return [
        jnp.broadcast_to(rows_ref[k : k + 1, :].astype(jnp.float32), (n, n)).T
        for k in range(count)
    ]


def prep_kernel(cap_ref, ids_ref, order_ref, probs_ref, grad_ref, tok_ref, x_ref, q_ref, facts_ref,
                *, experts):
    rows, width = tok_ref.shape
    routes = ids_ref.shape[0]
    lane = iota((rows, lanes), 1)
    lane_f = lane.astype(jnp.float32)
    order = jnp.broadcast_to(order_ref[...].astype(jnp.float32), (rows, rows))
    earlier = (order < order.T).astype(jnp.bfloat16)
    ids = columns_of(ids_ref, routes)
    chances = columns_of(probs_ref, routes)
    hits = [lane_f == i for i in ids]
    routed = sum(h.astype(jnp.float32) for h in hits)
    before = jnp.dot(earlier, routed.astype(jnp.bfloat16), preferred_element_type=jnp.float32)
    limit = jnp.zeros((rows, lanes), jnp.float32)
    for e in range(experts):
        limit = jnp.where(lane == e, cap_ref[e].astype(jnp.float32), limit)
    grad = grad_ref[...]
    scale = jnp.maximum(jnp.max(jnp.abs(grad), axis=1, keepdims=True), 1.0)
    q_ref[...] = (grad / scale).astype(jnp.bfloat16)
    facts = jnp.zeros((rows, lanes), jnp.float32)
    for k in range(routes):
        rank = jnp.sum(jnp.where(hits[k], before, 0.0), axis=1, keepdims=True)
        most = jnp.sum(jnp.where(hits[k], limit, 0.0), axis=1, keepdims=True)
        high, low = (p.astype(jnp.float32) for p in high_low(chances[k]))
        facts = jnp.where(lane == k, ids[k], facts)
        facts = jnp.where(lane == routes + k, jnp.where(rank < most, rank, -1.0), facts)
        facts = jnp.where(lane == 2 * routes + k, high, facts)
        facts = jnp.where(lane == 3 * routes + k, low, facts)
    high, low = (s.astype(jnp.float32) for s in high_low(scale))
    facts = jnp.where(lane == 4 * routes, high, facts)
    facts = jnp.where(lane == 4 * routes + 1, low, facts)
    x_ref[:, :width] = tok_ref[...]
    facts = facts.astype(jnp.bfloat16)
    x_ref[:, width:] = facts
    facts_ref[...] = facts


def chunks_of(place_ref, refs, outer, inner):
    if len(refs) == outer:
        return jnp.concatenate([r[...] for r in refs], axis=0)
    own, below, above, down, up, across = refs
    z = lax.div(place_ref[0], inner)
    back = jnp.where(z == 0, across[...], below[...])
    ahead = jnp.where(z == outer - 1, across[...], above[...])
    middle = jnp.where(z < outer // 2, down[...], up[...])
    return jnp.concatenate([own[...], back, middle, ahead], axis=0)


def partner(ep_rank, steps, places, outer, inner):
    z = lax.rem(lax.div(ep_rank, inner) + steps, outer)
    return (z * inner + lax.rem(lax.rem(ep_rank, inner) + places, inner)).astype(jnp.float32)


def x_slots_kernel(place_ref, *refs, outer, inner, capacity, routes):
    outs = refs[-inner - 1 :]
    rows = chunks_of(place_ref, refs[: -inner - 1], outer, inner)
    count, wide = rows.shape
    width = wide - lanes
    block = outer * capacity
    facts = rows[:, width:].astype(jnp.float32)
    chunk = (iota((count, 1), 0) // (count // outer)).astype(jnp.float32)
    slot = iota((count, inner * block), 1).astype(jnp.float32)
    table = jnp.zeros((count, inner * block), jnp.float32)
    chances = [jnp.zeros((count, 1), jnp.float32)] * inner
    for k in range(routes):
        expert = facts[:, k : k + 1]
        rank = facts[:, routes + k : routes + k + 1]
        prob = facts[:, 2 * routes + k : 2 * routes + k + 1]
        prob = prob + facts[:, 3 * routes + k : 3 * routes + k + 1]
        column = jnp.full((count, 1), -1.0, jnp.float32)
        for d in range(inner):
            mine = (expert == partner(place_ref[0], 0, d, outer, inner)) & (rank >= 0.0)
            column = jnp.where(mine, d * block + chunk * capacity + rank, column)
            chances[d] = jnp.where(mine, prob, chances[d])
        table = table + (slot == column).astype(jnp.float32)
    table = table.astype(jnp.bfloat16)
    outs[-1][...] = table
    lane = iota((count, lanes), 1)
    scales = jnp.where(
        lane == 2,
        facts[:, 4 * routes : 4 * routes + 1],
        jnp.where(lane == 3, facts[:, 4 * routes + 1 : 4 * routes + 2], 0.0),
    )
    for d in range(inner):
        part = table[:, d * block : (d + 1) * block]
        high, low = (h.astype(jnp.float32) for h in high_low(chances[d]))
        kept = jnp.where(lane == 0, high, jnp.where(lane == 1, low, scales)).astype(jnp.bfloat16)
        outs[d][:, :width] = contract_first(part, rows[:, :width]).astype(jnp.bfloat16)
        outs[d][:, width:] = contract_first(part, kept).astype(jnp.bfloat16)


def q_slots_kernel(place_ref, table_ref, *refs, outer, inner):
    outs = refs[-inner:]
    rows = chunks_of(place_ref, refs[:-inner], outer, inner)
    block = table_ref.shape[1] // inner
    for d in range(inner):
        part = table_ref[:, d * block : (d + 1) * block]
        outs[d][...] = contract_first(part, rows).astype(jnp.bfloat16)


def slot_facts(values):
    values = values.astype(jnp.float32)
    scale = lane_sum(values, 2, 4)
    return scale, scale * lane_sum(values, 0, 2)


class Copies:
    def __init__(self, sems):
        self.sems, self.count = sems, 0

    def start(self, source, target):
        copy = pltpu.make_async_copy(source, target, self.sems.at[self.count])
        copy.start()
        self.count += 1
        return copy


def wait_all(copies):
    for copy in copies:
        copy.wait()


def activation(gate_pre, up_pre):
    squash = jax.nn.sigmoid(sharpness * gate_pre)
    gated = gate_pre * squash
    more = up_pre + 1.0
    return gated, more * gated, more * (squash + sharpness * gated * (1.0 - squash))


def act_kernel(x_hbm, gate_hbm, up_hbm, *refs, tiles):
    outs_hbm, outs, (x, gate, up, sems, own_sems) = refs[:3], refs[3:6], refs[6:]
    size, width = gate.shape[1:]
    copies = Copies(own_sems)

    def tile_copy(i, tile):
        source, target = ((gate_hbm, gate), (up_hbm, up))[i]
        part = pl.ds(tile * size, size)
        return pltpu.make_async_copy(source.at[part, :], target.at[tile], sems.at[i, tile])

    load = copies.start(x_hbm, x)
    for tile in range(tiles):
        tile_copy(0, tile).start()
        tile_copy(1, tile).start()
    load.wait()

    def step(tile, carry):
        units = pl.ds(pl.multiple_of(tile * size, lanes), size)
        tile_copy(0, tile).wait()
        gate_pre = contract_last(x[:, :width], gate[tile])
        tile_copy(1, tile).wait()
        up_pre = contract_last(x[:, :width], up[tile])
        for out, term in zip(outs, activation(gate_pre, up_pre)):
            out[:, units] = term.astype(jnp.bfloat16)
        return carry

    lax.fori_loop(0, tiles, step, 0)
    wait_all([copies.start(out, out_hbm) for out, out_hbm in zip(outs, outs_hbm)])


def expert_kernel(rank_ref, x_hbm, q_hbm, *refs, tiles, known):
    weights_hbm, refs = refs[:3], refs[3:]
    terms_hbm, refs = (refs[:3], refs[3:]) if known else ((), refs)
    owns_hbm, refs = refs[:3], refs[3:]
    *refs, x, q, gate, up, down, every_gate, every_up, every_act, sum_ref, prob_ref, sems, own_sems = refs
    refs, terms = (refs[:-3], refs[-3:]) if known else (refs, ())
    outs_hbm, outs = refs[: len(refs) // 2], refs[len(refs) // 2 :]
    weights, alls = (gate, up, down), (every_gate, every_up, every_act)
    size, width = gate.shape[1:]
    copies = Copies(own_sems)

    def tile_copy(i, tile):
        part = pl.ds(tile * size, size)
        return pltpu.make_async_copy(
            weights_hbm[i].at[part, :], weights[i].at[tile], sems.at[i, tile]
        )

    order = (2, 0, 1) if known else (0, 1, 2)
    loads = [copies.start(q_hbm, q)] if known else [copies.start(x_hbm, x)]
    tile_copy(order[0], 0).start()
    facts_copy = None
    if known:
        facts_copy = copies.start(x_hbm.at[:, pl.ds(width, lanes)], x)
        loads += [copies.start(source, term) for source, term in zip(terms_hbm, terms)]
    else:
        loads.append(copies.start(q_hbm, q))
    tile_copy(order[1], 0).start()
    tile_copy(order[2], 0).start()
    for tile in range(1, tiles):
        for i in order:
            tile_copy(i, tile).start()
    if known:
        facts_copy.wait()
    wait_all(loads)
    scale, weight = slot_facts(x[...] if known else x[:, width:])
    sum_ref[...] = jnp.zeros_like(sum_ref)
    prob_ref[...] = jnp.zeros_like(prob_ref)

    def step(tile, carry):
        units = pl.ds(pl.multiple_of(tile * size, lanes), size)
        if known:
            gated, activated, slope = (t[:, units].astype(jnp.float32) for t in terms)
        else:
            tile_copy(0, tile).wait()
            gate_pre = contract_last(x[:, :width], gate[tile])
            tile_copy(1, tile).wait()
            gated, activated, slope = activation(
                gate_pre, contract_last(x[:, :width], up[tile])
            )
        tile_copy(2, tile).wait()
        back_proj = contract_last(q[...], down[tile])
        delta = weight * back_proj
        up_delta = (delta * gated).astype(jnp.bfloat16)
        gate_delta = (delta * slope).astype(jnp.bfloat16)
        every_gate[:, units] = gate_delta
        every_up[:, units] = up_delta
        every_act[:, units] = (activated * weight).astype(jnp.bfloat16)
        if known:
            tile_copy(0, tile).wait()
            tile_copy(1, tile).wait()
        share = jnp.dot(gate_delta, gate[tile], preferred_element_type=jnp.float32)
        share = share + jnp.dot(up_delta, up[tile], preferred_element_type=jnp.float32)
        sum_ref[...] += share
        prob_ref[...] += jnp.sum(activated * back_proj, axis=1, keepdims=True)
        return carry

    lax.fori_loop(0, tiles, step, 0)
    high, low = (h.astype(jnp.float32) for h in high_low(scale * prob_ref[...]))
    lane = iota((sum_ref.shape[0], lanes), 1)
    facts = jnp.where(lane == 0, high, jnp.where(lane == 1, low, 0.0))
    stores = []
    for i, (out, out_hbm) in enumerate(zip(outs, outs_hbm)):
        rows = out.shape[0]
        part = slice(i * rows, (i + 1) * rows)
        out[:, :width] = sum_ref[part, :].astype(jnp.bfloat16)
        out[:, width:] = facts[part].astype(jnp.bfloat16)
        stores.append(copies.start(out, out_hbm))
    quarter = owns_hbm[0].shape[1]
    mine = pl.ds(pl.multiple_of(rank_ref[0] * quarter, lanes), quarter)
    stores += [copies.start(every.at[:, mine], own) for every, own in zip(alls, owns_hbm)]
    wait_all(stores)


def weight_kernel(rank_ref, *refs, blocks, ready, rows, with_start):
    x_hbm, refs = refs[:blocks], refs[blocks:]
    q_hbm, refs = refs[:blocks], refs[blocks:]
    deltas_hbm, refs = refs[: 3 * ready], refs[3 * ready :]
    weights_hbm, refs = refs[:3], refs[3:]
    starts_hbm, refs = (refs[:3], refs[3:]) if with_start else ((), refs)
    outs_hbm, refs = refs[:3], refs[3:]
    x, q, gate_up, down, refs = *refs[:4], refs[4:]
    parts, sums, sems = refs[:3], refs[3:6], refs[6]
    copies = Copies(sems)
    quarter = down.shape[0]
    mine = pl.ds(rank_ref[0] * quarter, quarter)
    known = ready * rows
    place = lambda b: pl.ds(b * rows, rows)
    first = [copies.start(x_hbm[b], x.at[place(b)]) for b in range(ready, blocks)]
    for i in range(2):
        target = gate_up.at[pl.ds(i * quarter, quarter)]
        first.append(copies.start(weights_hbm[i].at[mine, :], target))
    second = [copies.start(q_hbm[b], q.at[place(b)]) for b in range(ready, blocks)]
    second.append(copies.start(weights_hbm[2].at[mine, :], down))
    third = []
    for b in range(ready):
        third += [copies.start(x_hbm[b], x.at[place(b)]), copies.start(q_hbm[b], q.at[place(b)])]
        third += [
            copies.start(deltas_hbm[3 * b + i], parts[i].at[place(b)]) for i in range(3)
        ]
    third += [copies.start(s, h) for s, h in zip(starts_hbm, sums)]
    wait_all(first)
    width = q.shape[1]
    pre = contract_last(x[known:, :width], gate_up[...])
    wait_all(second)
    back_proj = contract_last(q[known:], down[...])
    _, weight = slot_facts(x[known:, width:])
    gated, activated, slope = activation(pre[:, :quarter], pre[:, quarter:])
    delta = weight * back_proj
    parts[0][known:, :] = (delta * slope).astype(jnp.bfloat16)
    parts[1][known:, :] = (delta * gated).astype(jnp.bfloat16)
    parts[2][known:, :] = (activated * weight).astype(jnp.bfloat16)
    wait_all(third)
    stores = []
    for i, right in enumerate((x[:, :width], x[:, :width], q[...])):
        total = contract_first(parts[i][...], right)
        if with_start:
            total = total + sums[i][...].astype(jnp.float32)
        sums[i][...] = total.astype(jnp.bfloat16)
        stores.append(copies.start(sums[i], outs_hbm[i]))
    wait_all(stores)


def combine_kernel(place_ref, facts_ref, *refs, routes, outer, inner):
    backs, (grad_ref, prob_ref) = refs[:-2], refs[-2:]
    rows = facts_ref.shape[0]
    capacity, wide = backs[0].shape
    width = wide - lanes
    facts = facts_ref[...].astype(jnp.float32)
    slot = iota((rows, capacity), 1).astype(jnp.float32)
    lane = iota((rows, lanes), 1)
    total = jnp.zeros((rows, width), jnp.float32)
    pairs = jnp.zeros((rows, lanes), jnp.float32)
    for p, back in enumerate(backs):
        expert = partner(place_ref[0], p % outer, p // outer, outer, inner)
        table = jnp.zeros((rows, capacity), jnp.float32)
        where_k = jnp.zeros((rows, 1), jnp.float32) - 1.0
        for k in range(routes):
            mine = facts[:, k : k + 1] == expert
            rank = jnp.where(mine, facts[:, routes + k : routes + k + 1], -1.0)
            table = table + (slot == rank).astype(jnp.float32)
            where_k = jnp.where(mine, float(k), where_k)
        table = table.astype(jnp.bfloat16)
        total = total + jnp.dot(table, back[:, :width], preferred_element_type=jnp.float32)
        term = lane_sum(
            jnp.dot(table, back[:, width:], preferred_element_type=jnp.float32), 0, 2
        )
        pairs = pairs + jnp.where(lane.astype(jnp.float32) == where_k, term, 0.0)
    grad_ref[...] = total.astype(jnp.bfloat16)
    prob_ref[...] = pairs.T[:routes]


def on_device(
    grad_out, tokens, probs, expert_ids, priority, cap_counts, gate_weight, up_weight, down_weight,
    *, outer,
):
    ep_size = lax.axis_size("ep")
    dp_size = lax.axis_size("dp")
    inner = ep_size // outer
    ep_rank = lax.axis_index("ep").astype(jnp.int32)
    rank = lax.axis_index("dp").reshape(1).astype(jnp.int32)
    tok_rows, model_width = tokens.shape
    routes = expert_ids.shape[1]
    hidden = gate_weight.shape[1]
    quarter = hidden // dp_size
    capacity = 5 * routes * tok_rows // (4 * ep_size)
    block = outer * capacity
    wide = model_width + lanes
    w_gate, w_up, w_down = gate_weight[0], up_weight[0], down_weight[0]
    bf16, f32 = jnp.bfloat16, jnp.float32
    shape = jax.ShapeDtypeStruct
    vmem = pl.BlockSpec(memory_space=pltpu.VMEM)
    smem = pl.BlockSpec(memory_space=pltpu.SMEM)
    hbm = pl.BlockSpec(memory_space=pltpu.HBM)

    token_x, token_q, token_facts = pl.pallas_call(
        functools.partial(prep_kernel, experts=ep_size),
        out_shape=(
            shape((tok_rows, wide), bf16),
            shape((tok_rows, model_width), bf16),
            shape((tok_rows, lanes), bf16),
        ),
        in_specs=[smem] + [vmem] * 5,
        out_specs=(vmem,) * 3,
        compiler_params=pltpu.CompilerParams(vmem_limit_bytes=56 << 20),
        name="prep",
    )(cap_counts, expert_ids.T, priority, probs.T, grad_out, tokens)

    def move(rows, target):
        pairs = []
        for zz in range(outer):
            for i in range(inner):
                to = target(zz, i)
                if to is not None:
                    pairs.append((zz * inner + i, to[0] * inner + to[1]))
        return lax.ppermute(rows, "ep", pairs)

    def gather_near(rows):
        if outer != 4:
            return []
        below = move(rows, lambda zz, i: (zz + 1, i) if zz + 1 < outer else None)
        above = move(rows, lambda zz, i: (zz - 1, i) if zz else None)
        return [below, above]

    def gather_far(rows, near):
        if not near:
            back = lambda s: lambda zz, i: ((zz + s) % outer, i)
            return [rows] + [move(rows, back(s)) for s in range(1, outer)]
        below, above = near
        mixed = jnp.where(ep_rank < 2 * inner, below, above)
        across = move(mixed, lambda zz, i: {1: (3, i), 2: (0, i)}.get(zz))
        down = move(above, lambda zz, i: (zz - 1, i) if zz in (1, 2) else None)
        up = move(below, lambda zz, i: (zz + 1, i) if zz in (1, 2) else None)
        return [rows, below, above, down, up, across]

    spot = ep_rank.reshape(1)

    def x_slots(chunks):
        return pl.pallas_call(
            functools.partial(
                x_slots_kernel, outer=outer, inner=inner, capacity=capacity, routes=routes
            ),
            out_shape=(shape((block, wide), bf16),) * inner
            + (shape((outer * tok_rows, inner * block), bf16),),
            in_specs=[smem] + [vmem] * len(chunks),
            out_specs=(vmem,) * (inner + 1),
            compiler_params=pltpu.CompilerParams(vmem_limit_bytes=24 << 20),
            name="x_slots",
        )(spot, *chunks)

    def q_slots(table, chunks):
        return pl.pallas_call(
            functools.partial(q_slots_kernel, outer=outer, inner=inner),
            out_shape=(shape((block, model_width), bf16),) * inner,
            in_specs=[smem] + [vmem] * (1 + len(chunks)),
            out_specs=(vmem,) * inner,
            compiler_params=pltpu.CompilerParams(vmem_limit_bytes=24 << 20),
            name="q_slots",
        )(spot, table, *chunks)

    def exchange_inner(parts):
        step = lambda d: lambda zz, i: (zz, (i + d) % inner)
        got = [move(parts[d], step(d)) for d in range(1, inner)]
        return got[0] if inner == 2 else jnp.concatenate(got, axis=0)

    def swap(rows, step):
        return lax.ppermute(rows, "dp", [(d, d ^ step) for d in range(dp_size)])

    tiles = next(n for n in (3, 4, 2, 1) if hidden % (n * lanes) == 0)
    size = hidden // tiles

    def act_part(rows_x):
        count = rows_x.shape[0]
        return pl.pallas_call(
            functools.partial(act_kernel, tiles=tiles),
            in_specs=[hbm] * 3,
            out_specs=[hbm] * 3,
            scratch_shapes=[pltpu.VMEM((count, hidden), bf16)] * 3
            + [pltpu.VMEM((count, wide), bf16)]
            + [pltpu.VMEM((tiles, size, model_width), bf16)] * 2
            + [pltpu.SemaphoreType.DMA((2, tiles)), pltpu.SemaphoreType.DMA((4,))],
            out_shape=[pltpu.HBM((count, hidden), bf16)] * 3,
            compiler_params=pltpu.CompilerParams(vmem_limit_bytes=26 << 20),
            cost_estimate=pl.CostEstimate(
                flops=4 * count * model_width * hidden,
                bytes_accessed=4 * hidden * model_width,
                transcendentals=count * hidden,
            ),
            name="act_part",
        )(*in_hbm(rows_x, w_gate, w_up))

    def expert_part(rows_x, rows_q, terms):
        count = rows_q.shape[0]
        pieces = count // capacity
        loads = 5 + len(terms)
        results = pl.pallas_call(
            functools.partial(expert_kernel, tiles=tiles, known=bool(terms)),
            in_specs=[smem] + [hbm] * loads,
            out_specs=[hbm] * (3 + pieces),
            scratch_shapes=[pltpu.VMEM((capacity, wide), bf16)] * pieces
            + [pltpu.VMEM((count, hidden), bf16)] * len(terms)
            + [pltpu.VMEM((count, lanes if terms else wide), bf16)]
            + [pltpu.VMEM((count, model_width), bf16)]
            + [pltpu.VMEM((tiles, size, model_width), bf16)] * 3
            + [pltpu.VMEM((count, hidden), bf16)] * 3
            + [pltpu.VMEM((count, model_width), f32), pltpu.VMEM((count, 1), f32)]
            + [pltpu.SemaphoreType.DMA((3, tiles)), pltpu.SemaphoreType.DMA((pieces + loads,))],
            out_shape=[pltpu.HBM((count, quarter), bf16)] * 3
            + [pltpu.HBM((capacity, wide), bf16)] * pieces,
            compiler_params=pltpu.CompilerParams(vmem_limit_bytes=36 << 20),
            cost_estimate=pl.CostEstimate(
                flops=10 * count * model_width * hidden,
                bytes_accessed=6 * hidden * model_width,
                transcendentals=count * hidden,
            ),
            name="expert_part",
        )(rank, *in_hbm(rows_x, rows_q, w_gate, w_up, w_down, *terms))
        return results[:3], results[3:]

    def weight_grads(blocks_x, blocks_q, deltas, start):
        counts = [b.shape[0] for b in blocks_x]
        if len(set(counts)) > 1:
            size = math.gcd(*counts)
            cut = lambda bs: [b[i : i + size] for b in bs for i in range(0, b.shape[0], size)]
            blocks_x, blocks_q = cut(blocks_x), cut(blocks_q)
            if deltas:
                columns = [cut(c) for c in zip(*deltas)]
                deltas = list(zip(*columns))
        count, rows, ready = len(blocks_x), sum(counts), len(deltas)
        operands = [*blocks_x, *blocks_q, *sum(map(list, deltas), [])]
        operands += [w_gate, w_up, w_down, *(start or ())]
        scratch = [pltpu.VMEM((rows, wide), bf16), pltpu.VMEM((rows, model_width), bf16)]
        scratch += [pltpu.VMEM((2 * quarter, model_width), bf16)]
        scratch += [pltpu.VMEM((quarter, model_width), bf16)]
        scratch += [pltpu.VMEM((rows, quarter), bf16)] * 3
        scratch += [pltpu.VMEM((quarter, model_width), bf16)] * 3
        scratch += [pltpu.SemaphoreType.DMA((len(operands) + 3,))]
        return pl.pallas_call(
            functools.partial(
                weight_kernel,
                blocks=count,
                ready=ready,
                rows=rows // count,
                with_start=start is not None,
            ),
            out_shape=(pltpu.HBM((quarter, model_width), bf16),) * 3,
            in_specs=[smem] + [hbm] * len(operands),
            out_specs=(hbm,) * 3,
            scratch_shapes=scratch,
            compiler_params=pltpu.CompilerParams(vmem_limit_bytes=48 << 20),
            cost_estimate=pl.CostEstimate(
                flops=12 * rows * model_width * quarter,
                bytes_accessed=4 * rows * wide,
                transcendentals=rows * quarter,
            ),
            name="weight_grads",
        )(rank, *in_hbm(*operands))

    half = dp_size // 2

    def replicas(rows):
        near = [rows]
        far = [swap(rows, half)]
        step = half // 2
        while step:
            near += [swap(b, step) for b in near]
            far += [swap(b, step) for b in far]
            step //= 2
        return near, far

    near_chunks_x = gather_near(token_x)
    near_chunks_q = gather_near(token_q)
    chunks_x = gather_far(token_x, near_chunks_x)
    chunks_q = gather_far(token_q, near_chunks_q)
    *sends_x, table = x_slots(chunks_x)
    other_x = exchange_inner(sends_x)
    sends_q = q_slots(table, chunks_q)
    other_q = exchange_inner(sends_q)
    same_x, same_q = sends_x[0], sends_q[0]
    near_sx, far_sx = replicas(same_x)
    near_sq, far_sq = replicas(same_q)
    near_ox, far_ox = replicas(other_x)
    near_oq, far_oq = replicas(other_q)

    same_terms = act_part(same_x)
    same_deltas, same_back = expert_part(same_x, same_q, same_terms)
    other_deltas, other_back = expert_part(other_x, other_q, [])
    backs = []
    for i, rows in enumerate([*same_back, *other_back]):
        d, s = i // outer, i % outer
        if i:
            home = lambda zz, ii: ((zz - s) % outer, (ii - d) % inner)
            rows = move(rows, home)
        backs.append(rows)
    sums = weight_grads(near_sx, near_sq, [same_deltas], None)
    sums = weight_grads(near_ox + far_sx, near_oq + far_sq, [other_deltas], sums)
    shares = weight_grads(far_ox, far_oq, [], sums)
    input_grad, prob_grad = pl.pallas_call(
        functools.partial(combine_kernel, routes=routes, outer=outer, inner=inner),
        out_shape=(shape((tok_rows, model_width), bf16), shape((routes, tok_rows), f32)),
        in_specs=[smem] + [vmem] * (1 + len(backs)),
        out_specs=(vmem,) * 2,
        compiler_params=pltpu.CompilerParams(vmem_limit_bytes=24 << 20),
        name="combine",
    )(spot, token_facts, *backs)
    return (input_grad, prob_grad.T, *(share[None] for share in shares))


def outer_size(mesh):
    heights = {getattr(d, "coords", (0, 0, 0))[2] for d in mesh.devices.flat}
    return len(heights) if mesh.shape["ep"] % len(heights) == 0 else 1


def solution(mesh):
    def whole(*arrays):
        return on_device(*arrays, outer=outer_size(mesh))

    return jax.shard_map(
        whole,
        mesh=mesh,
        in_specs=(
            P(("ep", "dp"), None),
            P(("ep", "dp"), None),
            P(("ep", "dp"), None),
            P(("ep", "dp"), None),
            P(("ep", "dp"), None),
            P(),
            P("ep", None, None),
            P("ep", None, None),
            P("ep", None, None),
        ),
        out_specs=(
            P(("ep", "dp"), None),
            P(("ep", "dp"), None),
            P("ep", "dp", None),
            P("ep", "dp", None),
            P("ep", "dp", None),
        ),
        check_vma=False,
    )
```

```python
import functools
import math

import jax
import jax.numpy as jnp
from jax import lax
from jax.experimental import pallas as pl
from jax.experimental.pallas import tpu as pltpu
from jax.sharding import PartitionSpec as P


sharpness = 1.702
lanes = 128


def contract_last(first_op, second_op):
    return lax.dot_general(
        first_op, second_op, (((1,), (1,)), ((), ())), preferred_element_type=jnp.float32
    )


def contract_first(first_op, second_op):
    return lax.dot_general(
        first_op, second_op, (((0,), (0,)), ((), ())), preferred_element_type=jnp.float32
    )


def in_hbm(*arrays):
    return [pltpu.with_memory_space_constraint(a, pltpu.HBM) for a in arrays]


def high_low(values):
    high = values.astype(jnp.bfloat16)
    return high, (values - high.astype(jnp.float32)).astype(jnp.bfloat16)


def iota(shape, dim):
    return lax.broadcasted_iota(jnp.int32, shape, dim)


def lane_sum(values, first, stop):
    lane = iota(values.shape, 1)
    return jnp.sum(jnp.where((lane >= first) & (lane < stop), values, 0.0), axis=1, keepdims=True)


def columns_of(rows_ref, count):
    n = rows_ref.shape[1]
    return [
        jnp.broadcast_to(rows_ref[k : k + 1, :].astype(jnp.float32), (n, n)).T
        for k in range(count)
    ]


def prep_kernel(cap_ref, ids_ref, order_ref, probs_ref, grad_ref, tok_ref, x_ref, q_ref, facts_ref,
                *, experts):
    rows, width = tok_ref.shape
    routes = ids_ref.shape[0]
    lane = iota((rows, lanes), 1)
    lane_f = lane.astype(jnp.float32)
    order = jnp.broadcast_to(order_ref[...].astype(jnp.float32), (rows, rows))
    earlier = (order < order.T).astype(jnp.bfloat16)
    ids = columns_of(ids_ref, routes)
    chances = columns_of(probs_ref, routes)
    hits = [lane_f == i for i in ids]
    routed = sum(h.astype(jnp.float32) for h in hits)
    before = jnp.dot(earlier, routed.astype(jnp.bfloat16), preferred_element_type=jnp.float32)
    limit = jnp.zeros((rows, lanes), jnp.float32)
    for e in range(experts):
        limit = jnp.where(lane == e, cap_ref[e].astype(jnp.float32), limit)
    grad = grad_ref[...]
    scale = jnp.maximum(jnp.max(jnp.abs(grad), axis=1, keepdims=True), 1.0)
    q_ref[...] = (grad / scale).astype(jnp.bfloat16)
    facts = jnp.zeros((rows, lanes), jnp.float32)
    for k in range(routes):
        rank = jnp.sum(jnp.where(hits[k], before, 0.0), axis=1, keepdims=True)
        most = jnp.sum(jnp.where(hits[k], limit, 0.0), axis=1, keepdims=True)
        high, low = (p.astype(jnp.float32) for p in high_low(chances[k]))
        facts = jnp.where(lane == k, ids[k], facts)
        facts = jnp.where(lane == routes + k, jnp.where(rank < most, rank, -1.0), facts)
        facts = jnp.where(lane == 2 * routes + k, high, facts)
        facts = jnp.where(lane == 3 * routes + k, low, facts)
    high, low = (s.astype(jnp.float32) for s in high_low(scale))
    facts = jnp.where(lane == 4 * routes, high, facts)
    facts = jnp.where(lane == 4 * routes + 1, low, facts)
    x_ref[:, :width] = tok_ref[...]
    facts = facts.astype(jnp.bfloat16)
    x_ref[:, width:] = facts
    facts_ref[...] = facts


def chunks_of(place_ref, refs, outer, inner):
    if len(refs) == outer:
        return jnp.concatenate([r[...] for r in refs], axis=0)
    own, below, above, down, up, across = refs
    z = lax.div(place_ref[0], inner)
    back = jnp.where(z == 0, across[...], below[...])
    ahead = jnp.where(z == outer - 1, across[...], above[...])
    middle = jnp.where(z < outer // 2, down[...], up[...])
    return jnp.concatenate([own[...], back, middle, ahead], axis=0)


def partner(ep_rank, steps, places, outer, inner):
    z = lax.rem(lax.div(ep_rank, inner) + steps, outer)
    return (z * inner + lax.rem(lax.rem(ep_rank, inner) + places, inner)).astype(jnp.float32)


def x_slots_kernel(place_ref, *refs, outer, inner, capacity, routes):
    outs = refs[-inner - 1 :]
    rows = chunks_of(place_ref, refs[: -inner - 1], outer, inner)
    count, wide = rows.shape
    width = wide - lanes
    block = outer * capacity
    facts = rows[:, width:].astype(jnp.float32)
    chunk = (iota((count, 1), 0) // (count // outer)).astype(jnp.float32)
    slot = iota((count, inner * block), 1).astype(jnp.float32)
    table = jnp.zeros((count, inner * block), jnp.float32)
    chances = [jnp.zeros((count, 1), jnp.float32)] * inner
    for k in range(routes):
        expert = facts[:, k : k + 1]
        rank = facts[:, routes + k : routes + k + 1]
        prob = facts[:, 2 * routes + k : 2 * routes + k + 1]
        prob = prob + facts[:, 3 * routes + k : 3 * routes + k + 1]
        column = jnp.full((count, 1), -1.0, jnp.float32)
        for d in range(inner):
            mine = (expert == partner(place_ref[0], 0, d, outer, inner)) & (rank >= 0.0)
            column = jnp.where(mine, d * block + chunk * capacity + rank, column)
            chances[d] = jnp.where(mine, prob, chances[d])
        table = table + (slot == column).astype(jnp.float32)
    table = table.astype(jnp.bfloat16)
    outs[-1][...] = table
    lane = iota((count, lanes), 1)
    scales = jnp.where(
        lane == 2,
        facts[:, 4 * routes : 4 * routes + 1],
        jnp.where(lane == 3, facts[:, 4 * routes + 1 : 4 * routes + 2], 0.0),
    )
    for d in range(inner):
        part = table[:, d * block : (d + 1) * block]
        high, low = (h.astype(jnp.float32) for h in high_low(chances[d]))
        kept = jnp.where(lane == 0, high, jnp.where(lane == 1, low, scales)).astype(jnp.bfloat16)
        outs[d][:, :width] = contract_first(part, rows[:, :width]).astype(jnp.bfloat16)
        outs[d][:, width:] = contract_first(part, kept).astype(jnp.bfloat16)


def q_slots_kernel(place_ref, table_ref, *refs, outer, inner):
    outs = refs[-inner:]
    rows = chunks_of(place_ref, refs[:-inner], outer, inner)
    block = table_ref.shape[1] // inner
    for d in range(inner):
        part = table_ref[:, d * block : (d + 1) * block]
        outs[d][...] = contract_first(part, rows).astype(jnp.bfloat16)


def slot_facts(values):
    values = values.astype(jnp.float32)
    scale = lane_sum(values, 2, 4)
    return scale, scale * lane_sum(values, 0, 2)


class Copies:
    def __init__(self, sems):
        self.sems, self.count = sems, 0

    def start(self, source, target):
        copy = pltpu.make_async_copy(source, target, self.sems.at[self.count])
        copy.start()
        self.count += 1
        return copy


def wait_all(copies):
    for copy in copies:
        copy.wait()


def activation(gate_pre, up_pre):
    squash = jax.nn.sigmoid(sharpness * gate_pre)
    gated = gate_pre * squash
    more = up_pre + 1.0
    return gated, more * gated, more * (squash + sharpness * gated * (1.0 - squash))


def act_kernel(x_hbm, gate_hbm, up_hbm, *refs, tiles):
    outs_hbm, outs, (x, gate, up, sems, own_sems) = refs[:3], refs[3:6], refs[6:]
    size, width = gate.shape[1:]
    copies = Copies(own_sems)

    def tile_copy(i, tile):
        source, target = ((gate_hbm, gate), (up_hbm, up))[i]
        part = pl.ds(tile * size, size)
        return pltpu.make_async_copy(source.at[part, :], target.at[tile], sems.at[i, tile])

    load = copies.start(x_hbm, x)
    for tile in range(tiles):
        tile_copy(0, tile).start()
        tile_copy(1, tile).start()
    load.wait()

    def step(tile, carry):
        units = pl.ds(pl.multiple_of(tile * size, lanes), size)
        tile_copy(0, tile).wait()
        tile_copy(1, tile).wait()
        gate_pre = contract_last(x[:, :width], gate[tile])
        up_pre = contract_last(x[:, :width], up[tile])
        for out, term in zip(outs, activation(gate_pre, up_pre)):
            out[:, units] = term.astype(jnp.bfloat16)
        return carry

    lax.fori_loop(0, tiles, step, 0)
    wait_all([copies.start(out, out_hbm) for out, out_hbm in zip(outs, outs_hbm)])


def expert_kernel(rank_ref, x_hbm, q_hbm, *refs, tiles, known):
    weights_hbm, refs = refs[:3], refs[3:]
    terms_hbm, refs = (refs[:3], refs[3:]) if known else ((), refs)
    owns_hbm, refs = refs[:3], refs[3:]
    *refs, x, q, gate, up, down, every_gate, every_up, every_act, sum_ref, prob_ref, sems, own_sems = refs
    refs, terms = (refs[:-3], refs[-3:]) if known else (refs, ())
    outs_hbm, outs = refs[: len(refs) // 2], refs[len(refs) // 2 :]
    weights, alls = (gate, up, down), (every_gate, every_up, every_act)
    size, width = gate.shape[1:]
    copies = Copies(own_sems)

    def tile_copy(i, tile):
        part = pl.ds(tile * size, size)
        return pltpu.make_async_copy(
            weights_hbm[i].at[part, :], weights[i].at[tile], sems.at[i, tile]
        )

    order = (2, 0, 1) if known else (0, 1, 2)
    loads = [copies.start(q_hbm, q)] if known else [copies.start(x_hbm, x)]
    tile_copy(order[0], 0).start()
    facts_copy = None
    if known:
        facts_copy = copies.start(x_hbm.at[:, pl.ds(width, lanes)], x)
        loads += [copies.start(source, term) for source, term in zip(terms_hbm, terms)]
    else:
        loads.append(copies.start(q_hbm, q))
    tile_copy(order[1], 0).start()
    tile_copy(order[2], 0).start()
    for tile in range(1, tiles):
        for i in order:
            tile_copy(i, tile).start()
    if known:
        facts_copy.wait()
    wait_all(loads)
    scale, weight = slot_facts(x[...] if known else x[:, width:])
    sum_ref[...] = jnp.zeros_like(sum_ref)
    prob_ref[...] = jnp.zeros_like(prob_ref)

    def step(tile, carry):
        units = pl.ds(pl.multiple_of(tile * size, lanes), size)
        for i in range(3):
            tile_copy(i, tile).wait()
        if known:
            gated, activated, slope = (t[:, units].astype(jnp.float32) for t in terms)
        else:
            gate_pre = contract_last(x[:, :width], gate[tile])
            up_pre = contract_last(x[:, :width], up[tile])
            gated, activated, slope = activation(gate_pre, up_pre)
        back_proj = contract_last(q[...], down[tile])
        delta = weight * back_proj
        up_delta = (delta * gated).astype(jnp.bfloat16)
        gate_delta = (delta * slope).astype(jnp.bfloat16)
        every_gate[:, units] = gate_delta
        every_up[:, units] = up_delta
        every_act[:, units] = (activated * weight).astype(jnp.bfloat16)
        share = jnp.dot(gate_delta, gate[tile], preferred_element_type=jnp.float32)
        share = share + jnp.dot(up_delta, up[tile], preferred_element_type=jnp.float32)
        sum_ref[...] += share
        prob_ref[...] += jnp.sum(activated * back_proj, axis=1, keepdims=True)
        return carry

    lax.fori_loop(0, tiles, step, 0)
    high, low = (h.astype(jnp.float32) for h in high_low(scale * prob_ref[...]))
    lane = iota((sum_ref.shape[0], lanes), 1)
    facts = jnp.where(lane == 0, high, jnp.where(lane == 1, low, 0.0))
    stores = []
    for i, (out, out_hbm) in enumerate(zip(outs, outs_hbm)):
        rows = out.shape[0]
        part = slice(i * rows, (i + 1) * rows)
        out[:, :width] = sum_ref[part, :].astype(jnp.bfloat16)
        out[:, width:] = facts[part].astype(jnp.bfloat16)
        stores.append(copies.start(out, out_hbm))
    quarter = owns_hbm[0].shape[1]
    mine = pl.ds(pl.multiple_of(rank_ref[0] * quarter, lanes), quarter)
    stores += [copies.start(every.at[:, mine], own) for every, own in zip(alls, owns_hbm)]
    wait_all(stores)


def weight_kernel(rank_ref, *refs, blocks, ready, rows, with_start):
    x_hbm, refs = refs[:blocks], refs[blocks:]
    q_hbm, refs = refs[:blocks], refs[blocks:]
    deltas_hbm, refs = refs[: 3 * ready], refs[3 * ready :]
    weights_hbm, refs = refs[:3], refs[3:]
    starts_hbm, refs = (refs[:3], refs[3:]) if with_start else ((), refs)
    outs_hbm, refs = refs[:3], refs[3:]
    x, q, gate_up, down, refs = *refs[:4], refs[4:]
    parts, sums, sems = refs[:3], refs[3:6], refs[6]
    copies = Copies(sems)
    quarter = down.shape[0]
    mine = pl.ds(rank_ref[0] * quarter, quarter)
    known = ready * rows
    place = lambda b: pl.ds(b * rows, rows)
    first = [copies.start(x_hbm[b], x.at[place(b)]) for b in range(ready, blocks)]
    for i in range(2):
        target = gate_up.at[pl.ds(i * quarter, quarter)]
        first.append(copies.start(weights_hbm[i].at[mine, :], target))
    second = [copies.start(q_hbm[b], q.at[place(b)]) for b in range(ready, blocks)]
    second.append(copies.start(weights_hbm[2].at[mine, :], down))
    third = []
    for b in range(ready):
        third += [copies.start(x_hbm[b], x.at[place(b)]), copies.start(q_hbm[b], q.at[place(b)])]
        third += [
            copies.start(deltas_hbm[3 * b + i], parts[i].at[place(b)]) for i in range(3)
        ]
    third += [copies.start(s, h) for s, h in zip(starts_hbm, sums)]
    wait_all(first)
    width = q.shape[1]
    pre = contract_last(x[known:, :width], gate_up[...])
    wait_all(second)
    back_proj = contract_last(q[known:], down[...])
    _, weight = slot_facts(x[known:, width:])
    gated, activated, slope = activation(pre[:, :quarter], pre[:, quarter:])
    delta = weight * back_proj
    parts[0][known:, :] = (delta * slope).astype(jnp.bfloat16)
    parts[1][known:, :] = (delta * gated).astype(jnp.bfloat16)
    parts[2][known:, :] = (activated * weight).astype(jnp.bfloat16)
    wait_all(third)
    stores = []
    for i, right in enumerate((x[:, :width], x[:, :width], q[...])):
        total = contract_first(parts[i][...], right)
        if with_start:
            total = total + sums[i][...].astype(jnp.float32)
        sums[i][...] = total.astype(jnp.bfloat16)
        stores.append(copies.start(sums[i], outs_hbm[i]))
    wait_all(stores)


def combine_kernel(place_ref, facts_ref, *refs, routes, outer, inner):
    backs, (grad_ref, prob_ref) = refs[:-2], refs[-2:]
    rows = facts_ref.shape[0]
    capacity, wide = backs[0].shape
    width = wide - lanes
    facts = facts_ref[...].astype(jnp.float32)
    slot = iota((rows, capacity), 1).astype(jnp.float32)
    lane = iota((rows, lanes), 1)
    total = jnp.zeros((rows, width), jnp.float32)
    pairs = jnp.zeros((rows, lanes), jnp.float32)
    for p, back in enumerate(backs):
        expert = partner(place_ref[0], p % outer, p // outer, outer, inner)
        table = jnp.zeros((rows, capacity), jnp.float32)
        where_k = jnp.zeros((rows, 1), jnp.float32) - 1.0
        for k in range(routes):
            mine = facts[:, k : k + 1] == expert
            rank = jnp.where(mine, facts[:, routes + k : routes + k + 1], -1.0)
            table = table + (slot == rank).astype(jnp.float32)
            where_k = jnp.where(mine, float(k), where_k)
        table = table.astype(jnp.bfloat16)
        total = total + jnp.dot(table, back[:, :width], preferred_element_type=jnp.float32)
        term = lane_sum(
            jnp.dot(table, back[:, width:], preferred_element_type=jnp.float32), 0, 2
        )
        pairs = pairs + jnp.where(lane.astype(jnp.float32) == where_k, term, 0.0)
    grad_ref[...] = total.astype(jnp.bfloat16)
    prob_ref[...] = pairs.T[:routes]


def on_device(
    grad_out, tokens, probs, expert_ids, priority, cap_counts, gate_weight, up_weight, down_weight,
    *, outer,
):
    ep_size = lax.axis_size("ep")
    dp_size = lax.axis_size("dp")
    inner = ep_size // outer
    ep_rank = lax.axis_index("ep").astype(jnp.int32)
    rank = lax.axis_index("dp").reshape(1).astype(jnp.int32)
    tok_rows, model_width = tokens.shape
    routes = expert_ids.shape[1]
    hidden = gate_weight.shape[1]
    quarter = hidden // dp_size
    capacity = 5 * routes * tok_rows // (4 * ep_size)
    block = outer * capacity
    wide = model_width + lanes
    w_gate, w_up, w_down = gate_weight[0], up_weight[0], down_weight[0]
    bf16, f32 = jnp.bfloat16, jnp.float32
    shape = jax.ShapeDtypeStruct
    vmem = pl.BlockSpec(memory_space=pltpu.VMEM)
    smem = pl.BlockSpec(memory_space=pltpu.SMEM)
    hbm = pl.BlockSpec(memory_space=pltpu.HBM)

    token_x, token_q, token_facts = pl.pallas_call(
        functools.partial(prep_kernel, experts=ep_size),
        out_shape=(
            shape((tok_rows, wide), bf16),
            shape((tok_rows, model_width), bf16),
            shape((tok_rows, lanes), bf16),
        ),
        in_specs=[smem] + [vmem] * 5,
        out_specs=(vmem,) * 3,
        compiler_params=pltpu.CompilerParams(vmem_limit_bytes=56 << 20),
        name="prep",
    )(cap_counts, expert_ids.T, priority, probs.T, grad_out, tokens)

    def move(rows, target):
        pairs = []
        for zz in range(outer):
            for i in range(inner):
                to = target(zz, i)
                if to is not None:
                    pairs.append((zz * inner + i, to[0] * inner + to[1]))
        return lax.ppermute(rows, "ep", pairs)

    def gather_near(rows):
        if outer != 4:
            return []
        below = move(rows, lambda zz, i: (zz + 1, i) if zz + 1 < outer else None)
        above = move(rows, lambda zz, i: (zz - 1, i) if zz else None)
        return [below, above]

    def gather_far(rows, near):
        if not near:
            back = lambda s: lambda zz, i: ((zz + s) % outer, i)
            return [rows] + [move(rows, back(s)) for s in range(1, outer)]
        below, above = near
        mixed = jnp.where(ep_rank < 2 * inner, below, above)
        across = move(mixed, lambda zz, i: {1: (3, i), 2: (0, i)}.get(zz))
        down = move(above, lambda zz, i: (zz - 1, i) if zz in (1, 2) else None)
        up = move(below, lambda zz, i: (zz + 1, i) if zz in (1, 2) else None)
        return [rows, below, above, down, up, across]

    spot = ep_rank.reshape(1)

    def x_slots(chunks):
        return pl.pallas_call(
            functools.partial(
                x_slots_kernel, outer=outer, inner=inner, capacity=capacity, routes=routes
            ),
            out_shape=(shape((block, wide), bf16),) * inner
            + (shape((outer * tok_rows, inner * block), bf16),),
            in_specs=[smem] + [vmem] * len(chunks),
            out_specs=(vmem,) * (inner + 1),
            compiler_params=pltpu.CompilerParams(vmem_limit_bytes=24 << 20),
            name="x_slots",
        )(spot, *chunks)

    def q_slots(table, chunks):
        return pl.pallas_call(
            functools.partial(q_slots_kernel, outer=outer, inner=inner),
            out_shape=(shape((block, model_width), bf16),) * inner,
            in_specs=[smem] + [vmem] * (1 + len(chunks)),
            out_specs=(vmem,) * inner,
            compiler_params=pltpu.CompilerParams(vmem_limit_bytes=24 << 20),
            name="q_slots",
        )(spot, table, *chunks)

    def exchange_inner(parts):
        step = lambda d: lambda zz, i: (zz, (i + d) % inner)
        got = [move(parts[d], step(d)) for d in range(1, inner)]
        return got[0] if inner == 2 else jnp.concatenate(got, axis=0)

    def swap(rows, step):
        return lax.ppermute(rows, "dp", [(d, d ^ step) for d in range(dp_size)])

    tiles = next(n for n in (3, 4, 2, 1) if hidden % (n * lanes) == 0)
    size = hidden // tiles

    def act_part(rows_x):
        count = rows_x.shape[0]
        return pl.pallas_call(
            functools.partial(act_kernel, tiles=tiles),
            in_specs=[hbm] * 3,
            out_specs=[hbm] * 3,
            scratch_shapes=[pltpu.VMEM((count, hidden), bf16)] * 3
            + [pltpu.VMEM((count, wide), bf16)]
            + [pltpu.VMEM((tiles, size, model_width), bf16)] * 2
            + [pltpu.SemaphoreType.DMA((2, tiles)), pltpu.SemaphoreType.DMA((4,))],
            out_shape=[pltpu.HBM((count, hidden), bf16)] * 3,
            compiler_params=pltpu.CompilerParams(vmem_limit_bytes=48 << 20),
            cost_estimate=pl.CostEstimate(
                flops=4 * count * model_width * hidden,
                bytes_accessed=4 * hidden * model_width,
                transcendentals=count * hidden,
            ),
            name="act_part",
        )(rows_x, *in_hbm(w_gate, w_up))

    def expert_part(rows_x, rows_q, terms):
        count = rows_q.shape[0]
        pieces = count // capacity
        loads = 5 + len(terms)
        results = pl.pallas_call(
            functools.partial(expert_kernel, tiles=tiles, known=bool(terms)),
            in_specs=[smem] + [hbm] * loads,
            out_specs=[hbm] * (3 + pieces),
            scratch_shapes=[pltpu.VMEM((capacity, wide), bf16)] * pieces
            + [pltpu.VMEM((count, hidden), bf16)] * len(terms)
            + [pltpu.VMEM((count, lanes if terms else wide), bf16)]
            + [pltpu.VMEM((count, model_width), bf16)]
            + [pltpu.VMEM((tiles, size, model_width), bf16)] * 3
            + [pltpu.VMEM((count, hidden), bf16)] * 3
            + [pltpu.VMEM((count, model_width), f32), pltpu.VMEM((count, 1), f32)]
            + [pltpu.SemaphoreType.DMA((3, tiles)), pltpu.SemaphoreType.DMA((pieces + loads,))],
            out_shape=[pltpu.HBM((count, quarter), bf16)] * 3
            + [pltpu.HBM((capacity, wide), bf16)] * pieces,
            compiler_params=pltpu.CompilerParams(vmem_limit_bytes=48 << 20),
            cost_estimate=pl.CostEstimate(
                flops=10 * count * model_width * hidden,
                bytes_accessed=6 * hidden * model_width,
                transcendentals=count * hidden,
            ),
            name="expert_part",
        )(rank, rows_x, rows_q, *in_hbm(w_gate, w_up, w_down, *terms))
        return results[:3], results[3:]

    def weight_grads(blocks_x, blocks_q, deltas, start):
        counts = [b.shape[0] for b in blocks_x]
        if len(set(counts)) > 1:
            size = math.gcd(*counts)
            cut = lambda bs: [b[i : i + size] for b in bs for i in range(0, b.shape[0], size)]
            blocks_x, blocks_q = cut(blocks_x), cut(blocks_q)
            if deltas:
                columns = [cut(c) for c in zip(*deltas)]
                deltas = list(zip(*columns))
        count, rows, ready = len(blocks_x), sum(counts), len(deltas)
        kept = [*sum(map(list, deltas), []), w_gate, w_up, w_down, *(start or ())]
        operands = [*blocks_x, *blocks_q, *in_hbm(*kept)]
        scratch = [pltpu.VMEM((rows, wide), bf16), pltpu.VMEM((rows, model_width), bf16)]
        scratch += [pltpu.VMEM((2 * quarter, model_width), bf16)]
        scratch += [pltpu.VMEM((quarter, model_width), bf16)]
        scratch += [pltpu.VMEM((rows, quarter), bf16)] * 3
        scratch += [pltpu.VMEM((quarter, model_width), bf16)] * 3
        scratch += [pltpu.SemaphoreType.DMA((len(operands) + 3,))]
        return pl.pallas_call(
            functools.partial(
                weight_kernel,
                blocks=count,
                ready=ready,
                rows=rows // count,
                with_start=start is not None,
            ),
            out_shape=(pltpu.HBM((quarter, model_width), bf16),) * 3,
            in_specs=[smem] + [hbm] * len(operands),
            out_specs=(hbm,) * 3,
            scratch_shapes=scratch,
            compiler_params=pltpu.CompilerParams(vmem_limit_bytes=48 << 20),
            cost_estimate=pl.CostEstimate(
                flops=12 * rows * model_width * quarter,
                bytes_accessed=4 * rows * wide,
                transcendentals=rows * quarter,
            ),
            name="weight_grads",
        )(rank, *operands)

    half = dp_size // 2

    def replicas(rows):
        near = [rows]
        far = [swap(rows, half)]
        step = half // 2
        while step:
            near += [swap(b, step) for b in near]
            far += [swap(b, step) for b in far]
            step //= 2
        return near, far

    near_chunks_x = gather_near(token_x)
    near_chunks_q = gather_near(token_q)
    chunks_x = gather_far(token_x, near_chunks_x)
    chunks_q = gather_far(token_q, near_chunks_q)
    *sends_x, table = x_slots(chunks_x)
    other_x = exchange_inner(sends_x)
    sends_q = q_slots(table, chunks_q)
    other_q = exchange_inner(sends_q)
    same_x, same_q = sends_x[0], sends_q[0]
    near_sx, far_sx = replicas(same_x)
    near_sq, far_sq = replicas(same_q)
    near_ox, far_ox = replicas(other_x)
    near_oq, far_oq = replicas(other_q)

    same_terms = act_part(same_x)
    same_deltas, same_back = expert_part(same_x, same_q, same_terms)
    other_deltas, other_back = expert_part(other_x, other_q, [])
    backs = []
    for i, rows in enumerate([*same_back, *other_back]):
        d, s = i // outer, i % outer
        if i:
            home = lambda zz, ii: ((zz - s) % outer, (ii - d) % inner)
            rows = move(rows, home)
        backs.append(rows)
    sums = weight_grads(near_sx, near_sq, [same_deltas], None)
    sums = weight_grads(near_ox + far_sx, near_oq + far_sq, [other_deltas], sums)
    shares = weight_grads(far_ox, far_oq, [], sums)
    input_grad, prob_grad = pl.pallas_call(
        functools.partial(combine_kernel, routes=routes, outer=outer, inner=inner),
        out_shape=(shape((tok_rows, model_width), bf16), shape((routes, tok_rows), f32)),
        in_specs=[smem] + [vmem] * (1 + len(backs)),
        out_specs=(vmem,) * 2,
        compiler_params=pltpu.CompilerParams(vmem_limit_bytes=24 << 20),
        name="combine",
    )(spot, token_facts, *backs)
    return (input_grad, prob_grad.T, *(share[None] for share in shares))


def outer_size(mesh):
    heights = {getattr(d, "coords", (0, 0, 0))[2] for d in mesh.devices.flat}
    return len(heights) if mesh.shape["ep"] % len(heights) == 0 else 1


def solution(mesh):
    def whole(*arrays):
        return on_device(*arrays, outer=outer_size(mesh))

    return jax.shard_map(
        whole,
        mesh=mesh,
        in_specs=(
            P(("ep", "dp"), None),
            P(("ep", "dp"), None),
            P(("ep", "dp"), None),
            P(("ep", "dp"), None),
            P(("ep", "dp"), None),
            P(),
            P("ep", None, None),
            P("ep", None, None),
            P("ep", None, None),
        ),
        out_specs=(
            P(("ep", "dp"), None),
            P(("ep", "dp"), None),
            P("ep", "dp", None),
            P("ep", "dp", None),
            P("ep", "dp", None),
        ),
        check_vma=False,
    )
```

```python
import functools
import math

import jax
import jax.numpy as jnp
from jax import lax
from jax.experimental import pallas as pl
from jax.experimental.pallas import tpu as pltpu
from jax.sharding import PartitionSpec as P


sharpness = 1.702
lanes = 128


def contract_last(first_op, second_op):
    return lax.dot_general(
        first_op, second_op, (((1,), (1,)), ((), ())), preferred_element_type=jnp.float32
    )


def contract_first(first_op, second_op):
    return lax.dot_general(
        first_op, second_op, (((0,), (0,)), ((), ())), preferred_element_type=jnp.float32
    )


def in_hbm(*arrays):
    return [pltpu.with_memory_space_constraint(a, pltpu.HBM) for a in arrays]


def high_low(values):
    high = values.astype(jnp.bfloat16)
    return high, (values - high.astype(jnp.float32)).astype(jnp.bfloat16)


def iota(shape, dim):
    return lax.broadcasted_iota(jnp.int32, shape, dim)


def lane_sum(values, first, stop):
    lane = iota(values.shape, 1)
    return jnp.sum(jnp.where((lane >= first) & (lane < stop), values, 0.0), axis=1, keepdims=True)


def columns_of(rows_ref, count):
    n = rows_ref.shape[1]
    return [
        jnp.broadcast_to(rows_ref[k : k + 1, :].astype(jnp.float32), (n, n)).T
        for k in range(count)
    ]


def prep_kernel(cap_ref, ids_ref, order_ref, probs_ref, grad_ref, tok_ref, x_ref, q_ref, facts_ref,
                *, experts):
    rows, width = tok_ref.shape
    routes = ids_ref.shape[0]
    lane = iota((rows, lanes), 1)
    lane_f = lane.astype(jnp.float32)
    order = jnp.broadcast_to(order_ref[...].astype(jnp.float32), (rows, rows))
    earlier = (order < order.T).astype(jnp.bfloat16)
    ids = columns_of(ids_ref, routes)
    chances = columns_of(probs_ref, routes)
    hits = [lane_f == i for i in ids]
    routed = sum(h.astype(jnp.float32) for h in hits)
    before = jnp.dot(earlier, routed.astype(jnp.bfloat16), preferred_element_type=jnp.float32)
    limit = jnp.zeros((rows, lanes), jnp.float32)
    for e in range(experts):
        limit = jnp.where(lane == e, cap_ref[e].astype(jnp.float32), limit)
    grad = grad_ref[...]
    scale = jnp.maximum(jnp.max(jnp.abs(grad), axis=1, keepdims=True), 1.0)
    q_ref[...] = (grad / scale).astype(jnp.bfloat16)
    facts = jnp.zeros((rows, lanes), jnp.float32)
    for k in range(routes):
        rank = jnp.sum(jnp.where(hits[k], before, 0.0), axis=1, keepdims=True)
        most = jnp.sum(jnp.where(hits[k], limit, 0.0), axis=1, keepdims=True)
        high, low = (p.astype(jnp.float32) for p in high_low(chances[k]))
        facts = jnp.where(lane == k, ids[k], facts)
        facts = jnp.where(lane == routes + k, jnp.where(rank < most, rank, -1.0), facts)
        facts = jnp.where(lane == 2 * routes + k, high, facts)
        facts = jnp.where(lane == 3 * routes + k, low, facts)
    high, low = (s.astype(jnp.float32) for s in high_low(scale))
    facts = jnp.where(lane == 4 * routes, high, facts)
    facts = jnp.where(lane == 4 * routes + 1, low, facts)
    x_ref[:, :width] = tok_ref[...]
    facts = facts.astype(jnp.bfloat16)
    x_ref[:, width:] = facts
    facts_ref[...] = facts


def chunks_of(place_ref, refs, outer, inner):
    if len(refs) == outer:
        return jnp.concatenate([r[...] for r in refs], axis=0)
    own, below, above, down, up, across = refs
    z = lax.div(place_ref[0], inner)
    back = jnp.where(z == 0, across[...], below[...])
    ahead = jnp.where(z == outer - 1, across[...], above[...])
    middle = jnp.where(z < outer // 2, down[...], up[...])
    return jnp.concatenate([own[...], back, middle, ahead], axis=0)


def partner(ep_rank, steps, places, outer, inner):
    z = lax.rem(lax.div(ep_rank, inner) + steps, outer)
    return (z * inner + lax.rem(lax.rem(ep_rank, inner) + places, inner)).astype(jnp.float32)


def x_slots_kernel(place_ref, *refs, outer, inner, capacity, routes):
    outs = refs[-inner - 1 :]
    rows = chunks_of(place_ref, refs[: -inner - 1], outer, inner)
    count, wide = rows.shape
    width = wide - lanes
    block = outer * capacity
    facts = rows[:, width:].astype(jnp.float32)
    chunk = (iota((count, 1), 0) // (count // outer)).astype(jnp.float32)
    slot = iota((count, inner * block), 1).astype(jnp.float32)
    table = jnp.zeros((count, inner * block), jnp.float32)
    chances = [jnp.zeros((count, 1), jnp.float32)] * inner
    for k in range(routes):
        expert = facts[:, k : k + 1]
        rank = facts[:, routes + k : routes + k + 1]
        prob = facts[:, 2 * routes + k : 2 * routes + k + 1]
        prob = prob + facts[:, 3 * routes + k : 3 * routes + k + 1]
        column = jnp.full((count, 1), -1.0, jnp.float32)
        for d in range(inner):
            mine = (expert == partner(place_ref[0], 0, d, outer, inner)) & (rank >= 0.0)
            column = jnp.where(mine, d * block + chunk * capacity + rank, column)
            chances[d] = jnp.where(mine, prob, chances[d])
        table = table + (slot == column).astype(jnp.float32)
    table = table.astype(jnp.bfloat16)
    outs[-1][...] = table
    lane = iota((count, lanes), 1)
    scales = jnp.where(
        lane == 2,
        facts[:, 4 * routes : 4 * routes + 1],
        jnp.where(lane == 3, facts[:, 4 * routes + 1 : 4 * routes + 2], 0.0),
    )
    for d in range(inner):
        part = table[:, d * block : (d + 1) * block]
        high, low = (h.astype(jnp.float32) for h in high_low(chances[d]))
        kept = jnp.where(lane == 0, high, jnp.where(lane == 1, low, scales)).astype(jnp.bfloat16)
        outs[d][:, :width] = contract_first(part, rows[:, :width]).astype(jnp.bfloat16)
        outs[d][:, width:] = contract_first(part, kept).astype(jnp.bfloat16)


def q_slots_kernel(place_ref, table_ref, *refs, outer, inner):
    outs = refs[-inner:]
    rows = chunks_of(place_ref, refs[:-inner], outer, inner)
    block = table_ref.shape[1] // inner
    for d in range(inner):
        part = table_ref[:, d * block : (d + 1) * block]
        outs[d][...] = contract_first(part, rows).astype(jnp.bfloat16)


def slot_facts(values):
    values = values.astype(jnp.float32)
    scale = lane_sum(values, 2, 4)
    return scale, scale * lane_sum(values, 0, 2)


class Copies:
    def __init__(self, sems):
        self.sems, self.count = sems, 0

    def start(self, source, target):
        copy = pltpu.make_async_copy(source, target, self.sems.at[self.count])
        copy.start()
        self.count += 1
        return copy


def wait_all(copies):
    for copy in copies:
        copy.wait()


def activation(gate_pre, up_pre):
    squash = jax.nn.sigmoid(sharpness * gate_pre)
    gated = gate_pre * squash
    more = up_pre + 1.0
    return gated, more * gated, more * (squash + sharpness * gated * (1.0 - squash))


def act_kernel(x_hbm, gate_hbm, up_hbm, *refs, tiles):
    outs_hbm, outs, (x, gate, up, sems, own_sems) = refs[:3], refs[3:6], refs[6:]
    size, width = gate.shape[1:]
    copies = Copies(own_sems)

    def tile_copy(i, tile):
        source, target = ((gate_hbm, gate), (up_hbm, up))[i]
        part = pl.ds(tile * size, size)
        return pltpu.make_async_copy(source.at[part, :], target.at[tile], sems.at[i, tile])

    load = copies.start(x_hbm, x)
    for tile in range(tiles):
        tile_copy(0, tile).start()
        tile_copy(1, tile).start()
    load.wait()

    def step(tile, carry):
        units = pl.ds(pl.multiple_of(tile * size, lanes), size)
        tile_copy(0, tile).wait()
        tile_copy(1, tile).wait()
        gate_pre = contract_last(x[:, :width], gate[tile])
        up_pre = contract_last(x[:, :width], up[tile])
        for out, term in zip(outs, activation(gate_pre, up_pre)):
            out[:, units] = term.astype(jnp.bfloat16)
        return carry

    lax.fori_loop(0, tiles, step, 0)
    wait_all([copies.start(out, out_hbm) for out, out_hbm in zip(outs, outs_hbm)])


def expert_kernel(rank_ref, x_hbm, q_hbm, *refs, tiles, known):
    weights_hbm, refs = refs[:3], refs[3:]
    terms_hbm, refs = (refs[:3], refs[3:]) if known else ((), refs)
    owns_hbm, refs = refs[:3], refs[3:]
    *refs, x, q, gate, up, down, every_gate, every_up, every_act, sum_ref, prob_ref, sems, own_sems = refs
    refs, terms = (refs[:-3], refs[-3:]) if known else (refs, ())
    outs_hbm, outs = refs[: len(refs) // 2], refs[len(refs) // 2 :]
    weights, alls = (gate, up, down), (every_gate, every_up, every_act)
    size, width = gate.shape[1:]
    copies = Copies(own_sems)

    def tile_copy(i, tile):
        part = pl.ds(tile * size, size)
        return pltpu.make_async_copy(
            weights_hbm[i].at[part, :], weights[i].at[tile], sems.at[i, tile]
        )

    order = (2, 0, 1) if known else (0, 1, 2)
    loads = [copies.start(q_hbm, q)] if known else [copies.start(x_hbm, x)]
    tile_copy(order[0], 0).start()
    facts_copy = None
    if known:
        facts_copy = copies.start(x_hbm.at[:, pl.ds(width, lanes)], x)
        loads += [copies.start(source, term) for source, term in zip(terms_hbm, terms)]
    else:
        loads.append(copies.start(q_hbm, q))
    tile_copy(order[1], 0).start()
    tile_copy(order[2], 0).start()
    for tile in range(1, tiles):
        for i in order:
            tile_copy(i, tile).start()
    if known:
        facts_copy.wait()
    wait_all(loads)
    scale, weight = slot_facts(x[...] if known else x[:, width:])
    sum_ref[...] = jnp.zeros_like(sum_ref)
    prob_ref[...] = jnp.zeros_like(prob_ref)

    def step(tile, carry):
        units = pl.ds(pl.multiple_of(tile * size, lanes), size)
        if known:
            tile_copy(2, tile).wait()
            back_proj = contract_last(q[...], down[tile])
            tile_copy(0, tile).wait()
            tile_copy(1, tile).wait()
            gated, activated, slope = (t[:, units].astype(jnp.float32) for t in terms)
        else:
            rows = x[:, :width]
            tile_copy(0, tile).wait()
            gate_pre = contract_last(rows, gate[tile])
            tile_copy(1, tile).wait()
            up_pre = contract_last(rows, up[tile])
            tile_copy(2, tile).wait()
            back_proj = contract_last(q[...], down[tile])
            gated, activated, slope = activation(gate_pre, up_pre)
        delta = weight * back_proj
        up_delta = (delta * gated).astype(jnp.bfloat16)
        gate_delta = (delta * slope).astype(jnp.bfloat16)
        every_gate[:, units] = gate_delta
        every_up[:, units] = up_delta
        every_act[:, units] = (activated * weight).astype(jnp.bfloat16)
        share = jnp.dot(gate_delta, gate[tile], preferred_element_type=jnp.float32)
        share = share + jnp.dot(up_delta, up[tile], preferred_element_type=jnp.float32)
        sum_ref[...] += share
        prob_ref[...] += jnp.sum(activated * back_proj, axis=1, keepdims=True)
        return carry

    lax.fori_loop(0, tiles, step, 0)
    high, low = (h.astype(jnp.float32) for h in high_low(scale * prob_ref[...]))
    lane = iota((sum_ref.shape[0], lanes), 1)
    facts = jnp.where(lane == 0, high, jnp.where(lane == 1, low, 0.0))
    stores = []
    for i, (out, out_hbm) in enumerate(zip(outs, outs_hbm)):
        rows = out.shape[0]
        part = slice(i * rows, (i + 1) * rows)
        out[:, :width] = sum_ref[part, :].astype(jnp.bfloat16)
        out[:, width:] = facts[part].astype(jnp.bfloat16)
        stores.append(copies.start(out, out_hbm))
    quarter = owns_hbm[0].shape[1]
    mine = pl.ds(pl.multiple_of(rank_ref[0] * quarter, lanes), quarter)
    stores += [copies.start(every.at[:, mine], own) for every, own in zip(alls, owns_hbm)]
    wait_all(stores)


def weight_kernel(rank_ref, *refs, blocks, ready, rows, with_start):
    x_hbm, refs = refs[:blocks], refs[blocks:]
    q_hbm, refs = refs[:blocks], refs[blocks:]
    deltas_hbm, refs = refs[: 3 * ready], refs[3 * ready :]
    weights_hbm, refs = refs[:3], refs[3:]
    starts_hbm, refs = (refs[:3], refs[3:]) if with_start else ((), refs)
    outs_hbm, refs = refs[:3], refs[3:]
    x, q, gate_up, down, refs = *refs[:4], refs[4:]
    parts, sums, sems = refs[:3], refs[3:6], refs[6]
    copies = Copies(sems)
    quarter = down.shape[0]
    mine = pl.ds(rank_ref[0] * quarter, quarter)
    known = ready * rows
    place = lambda b: pl.ds(b * rows, rows)
    first = [copies.start(x_hbm[b], x.at[place(b)]) for b in range(ready, blocks)]
    for i in range(2):
        target = gate_up.at[pl.ds(i * quarter, quarter)]
        first.append(copies.start(weights_hbm[i].at[mine, :], target))
    second = [copies.start(q_hbm[b], q.at[place(b)]) for b in range(ready, blocks)]
    second.append(copies.start(weights_hbm[2].at[mine, :], down))
    third = []
    for b in range(ready):
        third += [copies.start(x_hbm[b], x.at[place(b)]), copies.start(q_hbm[b], q.at[place(b)])]
        third += [
            copies.start(deltas_hbm[3 * b + i], parts[i].at[place(b)]) for i in range(3)
        ]
    third += [copies.start(s, h) for s, h in zip(starts_hbm, sums)]
    wait_all(first)
    width = q.shape[1]
    pre = contract_last(x[known:, :width], gate_up[...])
    wait_all(second)
    back_proj = contract_last(q[known:], down[...])
    _, weight = slot_facts(x[known:, width:])
    gated, activated, slope = activation(pre[:, :quarter], pre[:, quarter:])
    delta = weight * back_proj
    parts[0][known:, :] = (delta * slope).astype(jnp.bfloat16)
    parts[1][known:, :] = (delta * gated).astype(jnp.bfloat16)
    parts[2][known:, :] = (activated * weight).astype(jnp.bfloat16)
    wait_all(third)
    stores = []
    for i, right in enumerate((x[:, :width], x[:, :width], q[...])):
        total = contract_first(parts[i][...], right)
        if with_start:
            total = total + sums[i][...].astype(jnp.float32)
        sums[i][...] = total.astype(jnp.bfloat16)
        stores.append(copies.start(sums[i], outs_hbm[i]))
    wait_all(stores)


def combine_kernel(place_ref, facts_ref, *refs, routes, outer, inner):
    backs, (grad_ref, prob_ref) = refs[:-2], refs[-2:]
    rows = facts_ref.shape[0]
    capacity, wide = backs[0].shape
    width = wide - lanes
    facts = facts_ref[...].astype(jnp.float32)
    slot = iota((rows, capacity), 1).astype(jnp.float32)
    lane = iota((rows, lanes), 1)
    total = jnp.zeros((rows, width), jnp.float32)
    pairs = jnp.zeros((rows, lanes), jnp.float32)
    for p, back in enumerate(backs):
        expert = partner(place_ref[0], p % outer, p // outer, outer, inner)
        table = jnp.zeros((rows, capacity), jnp.float32)
        where_k = jnp.zeros((rows, 1), jnp.float32) - 1.0
        for k in range(routes):
            mine = facts[:, k : k + 1] == expert
            rank = jnp.where(mine, facts[:, routes + k : routes + k + 1], -1.0)
            table = table + (slot == rank).astype(jnp.float32)
            where_k = jnp.where(mine, float(k), where_k)
        table = table.astype(jnp.bfloat16)
        total = total + jnp.dot(table, back[:, :width], preferred_element_type=jnp.float32)
        term = lane_sum(
            jnp.dot(table, back[:, width:], preferred_element_type=jnp.float32), 0, 2
        )
        pairs = pairs + jnp.where(lane.astype(jnp.float32) == where_k, term, 0.0)
    grad_ref[...] = total.astype(jnp.bfloat16)
    prob_ref[...] = pairs.T[:routes]


def on_device(
    grad_out, tokens, probs, expert_ids, priority, cap_counts, gate_weight, up_weight, down_weight,
    *, outer,
):
    ep_size = lax.axis_size("ep")
    dp_size = lax.axis_size("dp")
    inner = ep_size // outer
    ep_rank = lax.axis_index("ep").astype(jnp.int32)
    rank = lax.axis_index("dp").reshape(1).astype(jnp.int32)
    tok_rows, model_width = tokens.shape
    routes = expert_ids.shape[1]
    hidden = gate_weight.shape[1]
    quarter = hidden // dp_size
    capacity = 5 * routes * tok_rows // (4 * ep_size)
    block = outer * capacity
    wide = model_width + lanes
    w_gate, w_up, w_down = gate_weight[0], up_weight[0], down_weight[0]
    bf16, f32 = jnp.bfloat16, jnp.float32
    shape = jax.ShapeDtypeStruct
    vmem = pl.BlockSpec(memory_space=pltpu.VMEM)
    smem = pl.BlockSpec(memory_space=pltpu.SMEM)
    hbm = pl.BlockSpec(memory_space=pltpu.HBM)

    token_x, token_q, token_facts = pl.pallas_call(
        functools.partial(prep_kernel, experts=ep_size),
        out_shape=(
            shape((tok_rows, wide), bf16),
            shape((tok_rows, model_width), bf16),
            shape((tok_rows, lanes), bf16),
        ),
        in_specs=[smem] + [vmem] * 5,
        out_specs=(vmem,) * 3,
        compiler_params=pltpu.CompilerParams(vmem_limit_bytes=56 << 20),
        name="prep",
    )(cap_counts, expert_ids.T, priority, probs.T, grad_out, tokens)

    def move(rows, target):
        pairs = []
        for zz in range(outer):
            for i in range(inner):
                to = target(zz, i)
                if to is not None:
                    pairs.append((zz * inner + i, to[0] * inner + to[1]))
        return lax.ppermute(rows, "ep", pairs)

    def gather_near(rows):
        if outer != 4:
            return []
        below = move(rows, lambda zz, i: (zz + 1, i) if zz + 1 < outer else None)
        above = move(rows, lambda zz, i: (zz - 1, i) if zz else None)
        return [below, above]

    def gather_far(rows, near):
        if not near:
            back = lambda s: lambda zz, i: ((zz + s) % outer, i)
            return [rows] + [move(rows, back(s)) for s in range(1, outer)]
        below, above = near
        mixed = jnp.where(ep_rank < 2 * inner, below, above)
        across = move(mixed, lambda zz, i: {1: (3, i), 2: (0, i)}.get(zz))
        down = move(above, lambda zz, i: (zz - 1, i) if zz in (1, 2) else None)
        up = move(below, lambda zz, i: (zz + 1, i) if zz in (1, 2) else None)
        return [rows, below, above, down, up, across]

    spot = ep_rank.reshape(1)

    def x_slots(chunks):
        return pl.pallas_call(
            functools.partial(
                x_slots_kernel, outer=outer, inner=inner, capacity=capacity, routes=routes
            ),
            out_shape=(shape((block, wide), bf16),) * inner
            + (shape((outer * tok_rows, inner * block), bf16),),
            in_specs=[smem] + [vmem] * len(chunks),
            out_specs=(vmem,) * (inner + 1),
            compiler_params=pltpu.CompilerParams(vmem_limit_bytes=24 << 20),
            name="x_slots",
        )(spot, *chunks)

    def q_slots(table, chunks):
        return pl.pallas_call(
            functools.partial(q_slots_kernel, outer=outer, inner=inner),
            out_shape=(shape((block, model_width), bf16),) * inner,
            in_specs=[smem] + [vmem] * (1 + len(chunks)),
            out_specs=(vmem,) * inner,
            compiler_params=pltpu.CompilerParams(vmem_limit_bytes=24 << 20),
            name="q_slots",
        )(spot, table, *chunks)

    def exchange_inner(parts):
        step = lambda d: lambda zz, i: (zz, (i + d) % inner)
        got = [move(parts[d], step(d)) for d in range(1, inner)]
        return got[0] if inner == 2 else jnp.concatenate(got, axis=0)

    def swap(rows, step):
        return lax.ppermute(rows, "dp", [(d, d ^ step) for d in range(dp_size)])

    tiles = next(n for n in (3, 4, 2, 1) if hidden % (n * lanes) == 0)
    size = hidden // tiles

    def act_part(rows_x):
        count = rows_x.shape[0]
        return pl.pallas_call(
            functools.partial(act_kernel, tiles=tiles),
            in_specs=[hbm] * 3,
            out_specs=[hbm] * 3,
            scratch_shapes=[pltpu.VMEM((count, hidden), bf16)] * 3
            + [pltpu.VMEM((count, wide), bf16)]
            + [pltpu.VMEM((tiles, size, model_width), bf16)] * 2
            + [pltpu.SemaphoreType.DMA((2, tiles)), pltpu.SemaphoreType.DMA((4,))],
            out_shape=[pltpu.HBM((count, hidden), bf16)] * 3,
            compiler_params=pltpu.CompilerParams(vmem_limit_bytes=48 << 20),
            cost_estimate=pl.CostEstimate(
                flops=4 * count * model_width * hidden,
                bytes_accessed=4 * hidden * model_width,
                transcendentals=count * hidden,
            ),
            name="act_part",
        )(rows_x, *in_hbm(w_gate, w_up))

    def expert_part(rows_x, rows_q, terms):
        count = rows_q.shape[0]
        pieces = count // capacity
        loads = 5 + len(terms)
        results = pl.pallas_call(
            functools.partial(expert_kernel, tiles=tiles, known=bool(terms)),
            in_specs=[smem] + [hbm] * loads,
            out_specs=[hbm] * (3 + pieces),
            scratch_shapes=[pltpu.VMEM((capacity, wide), bf16)] * pieces
            + [pltpu.VMEM((count, hidden), bf16)] * len(terms)
            + [pltpu.VMEM((count, lanes if terms else wide), bf16)]
            + [pltpu.VMEM((count, model_width), bf16)]
            + [pltpu.VMEM((tiles, size, model_width), bf16)] * 3
            + [pltpu.VMEM((count, hidden), bf16)] * 3
            + [pltpu.VMEM((count, model_width), f32), pltpu.VMEM((count, 1), f32)]
            + [pltpu.SemaphoreType.DMA((3, tiles)), pltpu.SemaphoreType.DMA((pieces + loads,))],
            out_shape=[pltpu.HBM((count, quarter), bf16)] * 3
            + [pltpu.HBM((capacity, wide), bf16)] * pieces,
            compiler_params=pltpu.CompilerParams(vmem_limit_bytes=48 << 20),
            cost_estimate=pl.CostEstimate(
                flops=10 * count * model_width * hidden,
                bytes_accessed=6 * hidden * model_width,
                transcendentals=count * hidden,
            ),
            name="expert_part",
        )(rank, rows_x, rows_q, *in_hbm(w_gate, w_up, w_down, *terms))
        return results[:3], results[3:]

    def weight_grads(blocks_x, blocks_q, deltas, start):
        counts = [b.shape[0] for b in blocks_x]
        if len(set(counts)) > 1:
            size = math.gcd(*counts)
            cut = lambda bs: [b[i : i + size] for b in bs for i in range(0, b.shape[0], size)]
            blocks_x, blocks_q = cut(blocks_x), cut(blocks_q)
            if deltas:
                columns = [cut(c) for c in zip(*deltas)]
                deltas = list(zip(*columns))
        count, rows, ready = len(blocks_x), sum(counts), len(deltas)
        kept = [*sum(map(list, deltas), []), w_gate, w_up, w_down, *(start or ())]
        operands = [*blocks_x, *blocks_q, *in_hbm(*kept)]
        scratch = [pltpu.VMEM((rows, wide), bf16), pltpu.VMEM((rows, model_width), bf16)]
        scratch += [pltpu.VMEM((2 * quarter, model_width), bf16)]
        scratch += [pltpu.VMEM((quarter, model_width), bf16)]
        scratch += [pltpu.VMEM((rows, quarter), bf16)] * 3
        scratch += [pltpu.VMEM((quarter, model_width), bf16)] * 3
        scratch += [pltpu.SemaphoreType.DMA((len(operands) + 3,))]
        return pl.pallas_call(
            functools.partial(
                weight_kernel,
                blocks=count,
                ready=ready,
                rows=rows // count,
                with_start=start is not None,
            ),
            out_shape=(pltpu.HBM((quarter, model_width), bf16),) * 3,
            in_specs=[smem] + [hbm] * len(operands),
            out_specs=(hbm,) * 3,
            scratch_shapes=scratch,
            compiler_params=pltpu.CompilerParams(vmem_limit_bytes=48 << 20),
            cost_estimate=pl.CostEstimate(
                flops=12 * rows * model_width * quarter,
                bytes_accessed=4 * rows * wide,
                transcendentals=rows * quarter,
            ),
            name="weight_grads",
        )(rank, *operands)

    half = dp_size // 2

    def replicas(rows):
        near = [rows]
        far = [swap(rows, half)]
        step = half // 2
        while step:
            near += [swap(b, step) for b in near]
            far += [swap(b, step) for b in far]
            step //= 2
        return near, far

    near_chunks_x = gather_near(token_x)
    near_chunks_q = gather_near(token_q)
    chunks_x = gather_far(token_x, near_chunks_x)
    chunks_q = gather_far(token_q, near_chunks_q)
    *sends_x, table = x_slots(chunks_x)
    other_x = exchange_inner(sends_x)
    sends_q = q_slots(table, chunks_q)
    other_q = exchange_inner(sends_q)
    same_x, same_q = sends_x[0], sends_q[0]
    near_sx, far_sx = replicas(same_x)
    near_sq, far_sq = replicas(same_q)
    near_ox, far_ox = replicas(other_x)
    near_oq, far_oq = replicas(other_q)

    same_terms = act_part(same_x)
    same_deltas, same_back = expert_part(same_x, same_q, same_terms)
    other_deltas, other_back = expert_part(other_x, other_q, [])
    backs = []
    for i, rows in enumerate([*same_back, *other_back]):
        d, s = i // outer, i % outer
        if i:
            home = lambda zz, ii: ((zz - s) % outer, (ii - d) % inner)
            rows = move(rows, home)
        backs.append(rows)
    sums = weight_grads(near_sx, near_sq, [same_deltas], None)
    sums = weight_grads(near_ox + far_sx, near_oq + far_sq, [other_deltas], sums)
    shares = weight_grads(far_ox, far_oq, [], sums)
    input_grad, prob_grad = pl.pallas_call(
        functools.partial(combine_kernel, routes=routes, outer=outer, inner=inner),
        out_shape=(shape((tok_rows, model_width), bf16), shape((routes, tok_rows), f32)),
        in_specs=[smem] + [vmem] * (1 + len(backs)),
        out_specs=(vmem,) * 2,
        compiler_params=pltpu.CompilerParams(vmem_limit_bytes=24 << 20),
        name="combine",
    )(spot, token_facts, *backs)
    return (input_grad, prob_grad.T, *(share[None] for share in shares))


def outer_size(mesh):
    heights = {getattr(d, "coords", (0, 0, 0))[2] for d in mesh.devices.flat}
    return len(heights) if mesh.shape["ep"] % len(heights) == 0 else 1


def solution(mesh):
    def whole(*arrays):
        return on_device(*arrays, outer=outer_size(mesh))

    return jax.shard_map(
        whole,
        mesh=mesh,
        in_specs=(
            P(("ep", "dp"), None),
            P(("ep", "dp"), None),
            P(("ep", "dp"), None),
            P(("ep", "dp"), None),
            P(("ep", "dp"), None),
            P(),
            P("ep", None, None),
            P("ep", None, None),
            P("ep", None, None),
        ),
        out_specs=(
            P(("ep", "dp"), None),
            P(("ep", "dp"), None),
            P("ep", "dp", None),
            P("ep", "dp", None),
            P("ep", "dp", None),
        ),
        check_vma=False,
    )
```
